32 devices in a mesh: mkt: 8 (over z, x), grp: 4 (over y, core).
Axes of the slice: x: 2, y: 2, z: 4, core: 2. Of those that a mesh axis runs over, the one named last changes fastest.
Arguments:
- mean_utility: float32 [512, 64], P(('mkt', 'grp')), may hold values from -5 to -1
- market_share: float32 [512, 64], P(('mkt', 'grp')), may hold values from 0.001 to 0.02
- product_traits: float32 [512, 64, 5], P(('mkt', 'grp')), may hold values from -1 to 1
- taste_draws: float32 [512, 5, 1024], P(('mkt', 'grp')), may hold values from -4 to 4
- taste_scale: float32 [5], replicated, may hold values from 0.3 to 1
- type_weight: float32 [512, 1024], P(('mkt', 'grp')), may hold values from 0.1 to 1
- market_size: float32 [512], P(('mkt', 'grp')), may hold values from 0.05 to 3
- product_firm: int32 [512, 64], P(('mkt', 'grp')), may hold values from 0 to 511, all different within a row
- firm_order: int32 [512], replicated, may hold values from 0 to 511, each once
- loyalty: float32 [512, 1024], P(('mkt', 'grp')), may hold values from -1 to 1
- firm_share: float32 [512, 1024], replicated, may hold values from 2e-05 to 0.15
Outputs:
- utility_out: float32 [512, 64], P(('mkt', 'grp'))
- loyalty_out: float32 [512, 1024], P(('mkt', 'grp'))
The draws below stay inside these ranges and needn't reach their ends.
Inputs may be any that keep to these rules, and one draw needn't show every extreme that they name: `product_firm`: in each market the 64 products belong to 64 different firms, and every firm sells in some market. `firm_order`: each firm appears once.
All inputs are finite; a program needn't handle non-finite values.
Results may differ from the reference program's by a relative error of at most 0.0001.
Values sent between devices are 32-bit elements; how exact they have to be, the bound alone decides.
No kernel may reach another device: no remote copies, remote signals or barrier semaphores. Data moves between devices by JAX's collectives and lax.ppermute only.
A program may use at most 64 MiB of HBM per device.

```python
import math
import jax
import jax.numpy as jnp
from jax import lax

J = 64
FIRMS = 512
R = 1024
K = 5
ITERS = 3
M_DEV = 16
MARKETS = 512


def draw_market_size(key, part):
    index = jnp.arange(MARKETS, dtype=jnp.float32)
    base = 1.0 + 2.0 * index / max(MARKETS - 1, 1)
    factor = jnp.exp(jax.random.uniform(key, (MARKETS,), jnp.float32, jnp.log(0.05), 0.0))
    return base * factor


def draw_firm_share(key, part):
    key_firm = jax.random.fold_in(key, 11)
    key_type = jax.random.fold_in(key, 12)
    key_noise = jax.random.fold_in(key, 13)
    firm_level = jax.random.uniform(key_firm, (FIRMS, 1), jnp.float32, -2.5, 2.5)
    noise = jnp.clip(0.5 * jax.random.normal(key_noise, (FIRMS, R), jnp.float32), -1.0, 1.0)
    type_level = jax.random.uniform(key_type, (1, R), jnp.float32, -0.5, 0.5)
    return jnp.exp(-6.5 + firm_level + type_level + noise)


def shard_levels(stream_key, shape, cuts, low, high):
    level = 1.0
    for position, shards_of in cuts:
        draws = jax.random.uniform(jax.random.fold_in(jax.random.fold_in(stream_key, 6), position), (shards_of,), jnp.float32, low / len(cuts), high / len(cuts))
        level = level * jnp.repeat(jnp.exp(draws), shape[position] // shards_of).reshape((-1,) + (1,) * (len(shape) - 1 - position))
    return level


def distinct(own_key, rows, number_of, top, lift):
    ranking = jax.random.permutation(jax.random.fold_in(own_key, 1), number_of)
    pull = ranking
    for power in range(3):
        pull = pull * pull // number_of
    pull = pull * lift // number_of
    tickets = jax.random.randint(jax.random.fold_in(own_key, 2), (rows, number_of), 0, 4096) + pull
    fixed_rows = jax.random.permutation(jax.random.fold_in(own_key, 3), rows)[jnp.arange(number_of) % rows]
    tickets = jnp.where(jnp.arange(rows)[:, None] == fixed_rows[None, :], 1 << 14, tickets)
    score = tickets * number_of + jnp.arange(number_of)
    return lax.top_k(score.astype(jnp.int32), top)[1].astype(jnp.int32)


def scatter_about(stream_key, shape, spread, most, split=(), kind=jnp.bfloat16):
    level = shard_levels(stream_key, shape, split, -0.22, 0.18) if split else 1.0
    values = jax.random.normal(stream_key, shape, jnp.float32) * spread * level
    return jnp.minimum(jnp.maximum(values, -most), most).astype(kind)


def setup_inputs(seed: int = 0) -> dict:
    seeds = jax.random.split(jax.random.key(seed), 12)
    return {
        "mean_utility": jnp.clip(-5.0 + 4.0 * jax.random.uniform(seeds[0], (MARKETS, J), jnp.float32) ** shard_levels(seeds[0], (MARKETS, J), ((0, 32),), -0.2, 0.2), -5.0, -1.0),
        "market_share": jnp.clip(jnp.exp(math.log(0.02) - 2.9957322 * jax.random.uniform(seeds[1], (MARKETS, J), jnp.float32) ** shard_levels(seeds[1], (MARKETS, J), ((0, 32),), -0.2, 0.2)), 0.001, 0.02),
        "product_traits": jnp.clip(jax.random.uniform(seeds[2], (MARKETS, J, K), jnp.float32, -1.0, 1.0) * shard_levels(seeds[2], (MARKETS, J, K), ((0, 32),), -0.4, 0.0), -1.0, 1.0),
        "taste_draws": scatter_about(seeds[3], (MARKETS, K, R), 1.0, 4.0, ((0, 32),), jnp.float32),
        "taste_scale": jnp.clip(jnp.exp(jax.random.uniform(seeds[4], (K,), jnp.float32, math.log(0.3), math.log(1.0))), 0.3, 1.0),
        "type_weight": jnp.clip(jnp.exp(math.log(1.0) - 2.3025851 * jax.random.uniform(seeds[5], (MARKETS, R), jnp.float32) ** shard_levels(seeds[5], (MARKETS, R), ((0, 32),), -0.2, 0.2)), 0.1, 1.0),
        "market_size": draw_market_size(jax.random.fold_in(seeds[11], 71), 0),
        "product_firm": distinct(seeds[7], MARKETS, FIRMS, J, 1024),
        "firm_order": jax.random.permutation(seeds[8], FIRMS).astype(jnp.int32),
        "loyalty": jnp.clip(jax.random.uniform(seeds[9], (FIRMS, R), jnp.float32, -1.0, 1.0) * shard_levels(seeds[9], (FIRMS, R), ((0, 32),), -0.4, 0.0), -1.0, 1.0),
        "firm_share": draw_firm_share(jax.random.fold_in(seeds[11], 71), 0),
    }


clip_target = 0.5
norm_eps = 1e-06

def market_terms(mean_block, traits_block, draws_block, weight_block, size_block, firms_block, table, taste_scale):
    taste = jnp.einsum('mjk,mkr->mjr', traits_block * taste_scale, draws_block, precision=lax.Precision.HIGHEST)
    expu = jnp.exp(mean_block[:, :, None] + taste + jnp.take(table, firms_block, axis=0))
    choice_prob = expu / (1.0 + lax.optimization_barrier(jnp.sum(expu, axis=1, keepdims=True)))
    predicted = jnp.einsum('mjr,mr->mj', choice_prob, weight_block, precision=lax.Precision.HIGHEST) / lax.optimization_barrier(jnp.sum(weight_block, axis=1))[:, None]
    weighted = choice_prob * (size_block[:, None] * weight_block)[:, None, :]
    partial_value = jax.ops.segment_sum(weighted.reshape(-1, weighted.shape[2]), firms_block.reshape(-1), num_segments=table.shape[0])
    return (predicted, partial_value)

def reference(mean_utility, market_share, product_traits, taste_draws, taste_scale, type_weight, market_size, product_firm, firm_order, loyalty, firm_share):
    blocks = MARKETS // M_DEV
    table = jnp.zeros((FIRMS, R), loyalty.dtype).at[firm_order].set(loyalty)
    type_mass = lax.optimization_barrier(jnp.sum(market_size[:, None] * type_weight, axis=0))
    traits_b = product_traits.reshape(blocks, M_DEV, J, K)
    draws_b = taste_draws.reshape(blocks, M_DEV, K, R)
    weight_b = type_weight.reshape(blocks, M_DEV, R)
    size_b = market_size.reshape(blocks, M_DEV)
    firms_b = product_firm.reshape(blocks, M_DEV, J)
    mean_now = mean_utility
    for step in range(ITERS):
        mean_b = mean_now.reshape(blocks, M_DEV, J)

        def scan_block(carry, pieces):
            predicted, partial_value = market_terms(pieces[0], pieces[1], pieces[2], pieces[3], pieces[4], pieces[5], table, taste_scale)
            return (carry + partial_value, predicted)
        totals, predicted = lax.scan(scan_block, jnp.zeros((FIRMS, R), jnp.float32), (mean_b, traits_b, draws_b, weight_b, size_b, firms_b))
        gap = jnp.log(firm_share) - jnp.log(totals / type_mass[None, :])
        clip = jnp.minimum(1.0, clip_target / jnp.sqrt(jnp.mean(gap * gap) + norm_eps))
        table = table + clip * gap
        mean_now = mean_now + jnp.log(market_share) - jnp.log(predicted.reshape(MARKETS, J))
    return (mean_now, jnp.take(table, firm_order, axis=0))
```

```python
import functools

import jax
import jax.numpy as jnp
from jax import lax
from jax.experimental import pallas as pl
from jax.experimental.pallas import tpu as pltpu
from jax.sharding import PartitionSpec as P

ITERS = 3
LANES = 128
clip_target = 0.5
norm_eps = 1e-06
AXES = ("mkt", "grp")
BF = jnp.bfloat16
F32 = jnp.float32


class Plan:
    def __init__(self, devices, own_markets, products, traits, types, firms, own_firms):
        self.D = devices
        self.C = devices // 2
        self.M = own_markets
        self.J = products
        self.K = traits
        self.R = types
        self.F = firms
        self.own = own_firms
        self.RL = types // self.C
        self.hh = LANES // self.RL
        self.ii = own_markets // self.hh
        self.h = LANES // products
        self.i8 = own_markets // self.h
        self.g = self.i8 // self.ii
        self.ML = own_markets * self.C
        self.G = self.g * LANES
        self.FP = firms // self.hh
        self.ownp = -(-own_firms // self.hh) * self.hh
        self.oi = self.ownp // self.hh
        self.OR = self.C * self.oi
        self.s_draws = 0
        self.s_mass = self.s_draws + traits * self.ii
        self.s_traits = self.s_mass + self.ii
        self.s_firms = self.s_traits + traits * self.i8
        self.s_mean = self.s_firms + self.i8
        self.s_loy = self.s_mean + self.i8
        self.S = self.s_loy + self.oi
        self.S2 = self.i8 + 1
        self.S3 = self.i8 + 2 * self.oi + 1
        self.groups = [[2 * c + k for c in range(self.C)] for k in range(2)]
        self.swap = [(d, d ^ 1) for d in range(devices)]
        self.NR = max(LANES, 2 * self.RL)


VM = pl.BlockSpec(memory_space=pltpu.VMEM)


def call(kernel, outs, args, scratch=(), alias=None, vmem=48):
    return pl.pallas_call(
        kernel,
        out_shape=outs,
        in_specs=[VM] * len(args),
        out_specs=jax.tree.map(lambda _: VM, outs),
        scratch_shapes=list(scratch),
        input_output_aliases=alias or {},
        compiler_params=pltpu.CompilerParams(vmem_limit_bytes=vmem * 2**20),
    )(*args)


def sds(shape, dtype=F32):
    return jax.ShapeDtypeStruct(shape, dtype)


def block_mask(p, rows, b):
    lane = lax.broadcasted_iota(jnp.int32, (rows, LANES), 1)
    return lane // p.RL == b


def fold(p, x):
    total = x
    for b in range(1, p.hh):
        total = total + pltpu.roll(x, b * p.RL, 1)
    return total


def split3(x):
    a = x.astype(BF)
    rest = x - a.astype(F32)
    b = rest.astype(BF)
    c = (rest - b.astype(F32)).astype(BF)
    return a, b, c


def dot(a, b):
    return jnp.dot(a, b, preferred_element_type=F32)


def natural(p, src, dst, step, offset):
    for gi in range(p.g):
        for c in range(p.C):
            at = (gi * p.C + c) * p.ii
            dst[at : at + p.ii, :] = src[c * step + offset + gi * p.ii : c * step + offset + (gi + 1) * p.ii, :]


def turn(p, nat, store):
    for gi in range(p.g):
        turned = nat[gi * LANES : (gi + 1) * LANES, :].T
        for q in range(p.h):
            store(q * p.g + gi, turned[q * p.J : (q + 1) * p.J, :])


def firm_row(p, firms_t, j):
    return jnp.concatenate([firms_t[b, pl.ds(j, 1), :] for b in range(p.hh)], axis=1)


def pack_kernel(p, draws, mass, traits, firms, mean, loyalty, out):
    def by_type(x, section, rows, count):
        for t in range(p.R // LANES):
            tile = x[:, t * LANES : (t + 1) * LANES]
            for b in range(p.hh):
                c = t * p.hh + b
                value = None
                for q in range(p.hh):
                    shift = ((q - b) * p.RL) % LANES
                    moved = pltpu.roll(tile, shift, 1) if shift else tile
                    piece = moved[q * rows : (q + 1) * rows, :]
                    value = piece if value is None else jnp.where(block_mask(p, rows, q), piece, value)
                out[c * p.S + section : c * p.S + section + rows, :] = value

    for k in range(p.K):
        by_type(draws[k], p.s_draws + k * p.ii, p.ii, p.M)
    by_type(mass[...], p.s_mass, p.ii, p.M)
    by_type(loyalty[...], p.s_loy, p.oi, p.ownp)

    def copied(x, section):
        value = jnp.concatenate([x[q * p.i8 : (q + 1) * p.i8, :] for q in range(p.h)], axis=1)
        for c in range(p.C):
            out[c * p.S + section : c * p.S + section + p.i8, :] = value

    for k in range(p.K):
        copied(traits[k], p.s_traits + k * p.i8)
    copied(firms[...], p.s_firms)
    copied(mean[...], p.s_mean)


def prep_kernel(p, recv, taste, firms_t, mean_t, mass_t, mass_row, loy, nat, draws_t, traits_t):
    def typed(section, store):
        for c in range(p.C):
            nat[c * p.ii : (c + 1) * p.ii, :] = recv[c * p.S + section : c * p.S + section + p.ii, :]
        flat = nat[0:LANES, :]
        turned = flat.T
        for b in range(p.hh):
            store(b, turned[b * p.RL : (b + 1) * p.RL, :])
        return flat

    def put_mass(b, value):
        mass_t[:, b * LANES : (b + 1) * LANES] = value

    flat = typed(p.s_mass, put_mass)
    row = jnp.sum(flat, axis=0, keepdims=True)
    mass_row[...] = jnp.broadcast_to(fold(p, jnp.broadcast_to(row, (8, LANES))), (8, LANES))
    for k in range(p.K):

        def put_draws(b, value):
            draws_t[k, :, b * LANES : (b + 1) * LANES] = value

        typed(p.s_draws + k * p.ii, put_draws)

    def product(section, store):
        natural(p, recv, nat, p.S, section)
        turn(p, nat, store)

    def put_firms(b, value):
        firms_t[b] = value.astype(jnp.int32)

    def put_mean(b, value):
        mean_t[b] = value

    product(p.s_firms, put_firms)
    product(p.s_mean, put_mean)
    for k in range(p.K):

        def put_traits(b, value):
            traits_t[k, b] = value

        product(p.s_traits + k * p.i8, put_traits)
    for c in range(p.C):
        loy[c * p.oi : (c + 1) * p.oi, :] = recv[c * p.S + p.s_loy : c * p.S + p.s_loy + p.oi, :]

    def body(j, _):
        for b in range(p.hh):
            at = slice(b * LANES, (b + 1) * LANES)
            value = None
            for k in range(p.K):
                term = traits_t[k, b, pl.ds(j, 1), :] * draws_t[k, :, at]
                value = term if value is None else value + term
            taste[j, :, at] = value
        return 0

    lax.fori_loop(0, p.J, body, 0)


def table_kernel(p, mine, other, order, table):
    firm = lax.broadcasted_iota(jnp.int32, (p.F, p.OR), 0)
    total = jnp.zeros((p.F, LANES), F32)
    for s, ref in enumerate((mine, other)):
        pieces = split3(ref[...])
        for b in range(p.hh):
            hot = (firm == order[s * p.hh + b : s * p.hh + b + 1, :]).astype(BF)
            found = dot(hot, pieces[0]) + dot(hot, pieces[1]) + dot(hot, pieces[2])
            total = total + jnp.where(block_mask(p, p.F, b), found, 0.0)
    pack_table(p, fold(p, total), table)


def pack_table(p, full, out):
    value = full[0 : p.FP, :]
    for b in range(1, p.hh):
        value = jnp.where(block_mask(p, p.FP, b), full[b * p.FP : (b + 1) * p.FP, :], value)
    out[...] = value


def gather_kernel(p, packed, firms_t, out, tab):
    pieces = split3(packed[...].T)
    for b in range(p.hh):
        for q in range(3):
            tab[b, q * p.RL : (q + 1) * p.RL, :] = pieces[q][b * p.RL : (b + 1) * p.RL, :]

    def body(j, _):
        row = firm_row(p, firms_t, j)
        total = None
        for b in range(p.hh):
            firm = lax.broadcasted_iota(jnp.int32, (p.FP, p.ML), 0)
            hot = (firm == row - b * p.FP).astype(BF)
            term = dot(tab[b], hot)
            total = term if total is None else total + term
        out[j] = total[0 : p.RL] + total[p.RL : 2 * p.RL] + total[2 * p.RL : 3 * p.RL]
        return 0

    lax.fori_loop(0, p.J, body, 0, unroll=2)


def choice_body(p, utility_of, mass_t, parts, pred, expu, pred_t, base):
    for b in range(p.hh):
        at = slice(b * LANES, (b + 1) * LANES)

        def first(j, total):
            e = jnp.exp(utility_of(j, b, at))
            expu[j] = e
            return total + e

        total = lax.fori_loop(0, p.J, first, jnp.zeros((p.RL, LANES), F32), unroll=4)
        scale = mass_t[:, at] / (1.0 + total)

        def second(j, _):
            value = expu[j] * scale
            hi = value.astype(BF)
            parts[j, 0 : p.RL, at] = hi
            parts[j, p.RL : 2 * p.RL, at] = (value - hi.astype(F32)).astype(BF)
            if p.NR > 2 * p.RL:
                parts[j, 2 * p.RL :, at] = jnp.zeros((p.NR - 2 * p.RL, LANES), BF)
            pred_t[b, pl.ds(j, 1), :] = jnp.sum(value, axis=0, keepdims=True)
            return 0

        lax.fori_loop(0, p.J, second, 0, unroll=4)
    for gi in range(p.g):
        flat = jnp.concatenate([pred_t[q * p.g + gi] for q in range(p.h)], axis=0).T
        for c in range(p.C):
            pred[c * p.i8 + gi * p.ii : c * p.i8 + (gi + 1) * p.ii, :] = flat[c * p.ii : (c + 1) * p.ii, :]


def choice_first_kernel(p, taste, found, mean_t, mass_t, base, parts, pred, expu, pred_t):
    def utility_of(j, b, at):
        value = taste[j, :, at] + found[j, :, at]
        base[j, :, at] = value
        return value + mean_t[b, pl.ds(j, 1), :]

    choice_body(p, utility_of, mass_t, parts, pred, expu, pred_t, base)


def clip_of(p, squares):
    return jnp.minimum(1.0, clip_target / jnp.sqrt(squares / (p.F * p.R) + norm_eps))


def choice_next_kernel(p, base_in, found, recv, mass_t, base, parts, pred, clip, expu, pred_t, nat):
    natural(p, recv, nat, p.S2, 0)
    squares = recv[p.i8 : p.i8 + 1, :]
    for c in range(1, p.C):
        squares = squares + recv[c * p.S2 + p.i8 : c * p.S2 + p.i8 + 1, :]
    factor = clip_of(p, squares)
    clip[...] = jnp.broadcast_to(factor, (8, LANES))

    def put_mean(b, value):
        pred_t[b] = value

    turn(p, nat, put_mean)

    def utility_of(j, b, at):
        value = base_in[j, :, at] + factor * found[j, :, at]
        base[j, :, at] = value
        return value + pred_t[b, pl.ds(j, 1), :]

    choice_body(p, utility_of, mass_t, parts, pred, expu, pred_t, base)


def scatter_kernel(p, parts, firms_t, mass_row, out, acc):
    acc[...] = jnp.zeros_like(acc)
    firm = lax.broadcasted_iota(jnp.int32, (p.F, p.ML), 0)

    def body(j, _):
        value = None
        for u in range(2):
            hot = (firm == firm_row(p, firms_t, 2 * j + u)).astype(BF)
            term = lax.dot_general(hot, parts[2 * j + u], (((1,), (1,)), ((), ())), preferred_element_type=F32)
            value = term if value is None else value + term
        acc[...] += value
        return 0

    lax.fori_loop(0, p.J // 2, body, 0)
    pack_table(p, fold(p, acc[...]), out.at[0 : p.FP])
    out[p.FP : p.FP + 8, :] = mass_row[...]


def gap_of(p, mine, other, share):
    mass = mine[p.FP : p.FP + 1, :] + other[p.FP : p.FP + 1, :]
    totals = mine[0 : p.FP, :] + other[0 : p.FP, :]
    return jnp.log(share[...]) - jnp.log(totals / mass)


def squares_row(gap):
    rows = jnp.sum(gap * gap, axis=0, keepdims=True)
    return jnp.broadcast_to(jnp.sum(rows, axis=1, keepdims=True), (8, LANES))


def gap_kernel(p, mine, other, share, gap, squares):
    value = gap_of(p, mine, other, share)
    gap[...] = value
    squares[...] = squares_row(value)


def chunk_sum(p, recv, step, rows):
    total = recv[0:rows, :]
    for c in range(1, p.C):
        total = total + recv[c * step : c * step + rows, :]
    return total


def mean_kernel(p, recv, mean, log_share, mass_total, squares, mean_out, send):
    predicted = chunk_sum(p, recv, p.i8, p.i8) / mass_total[...]
    value = mean[...] + log_share[...] - jnp.log(predicted)
    mean_out[...] = value
    for c in range(p.C):
        send[c * p.S2 : c * p.S2 + p.i8, :] = value
        send[c * p.S2 + p.i8 : (c + 1) * p.S2, :] = squares[0:1, :]


def final_kernel(p, mine, other, share, table, gap0, gap1, clips, order, pred, send):
    gap = gap_of(p, mine, other, share)
    squares = squares_row(gap)
    base = table[...] + clips[0:1, :] * gap0[...] + clips[8:9, :] * gap1[...]
    rows = p.OR
    for n, value in enumerate((base, gap)):
        pieces = split3(value)
        picked = jnp.zeros((rows, LANES), F32)
        for o in range(p.hh):
            column = order[:, o : o + 1]
            total = jnp.zeros((rows, LANES), F32)
            for b in range(p.hh):
                firm = lax.broadcasted_iota(jnp.int32, (rows, p.FP), 1) + b * p.FP
                hot = (firm == column).astype(BF)
                found = dot(hot, pieces[0]) + dot(hot, pieces[1]) + dot(hot, pieces[2])
                total = total + jnp.where(block_mask(p, rows, b), found, 0.0)
            picked = jnp.where(block_mask(p, rows, o), fold(p, total), picked)
        at = p.i8 + n * p.oi
        for c in range(p.C):
            send[c * p.S3 + at : c * p.S3 + at + p.oi, :] = picked[c * p.oi : (c + 1) * p.oi, :]
    for c in range(p.C):
        send[c * p.S3 : c * p.S3 + p.i8, :] = pred[c * p.i8 : (c + 1) * p.i8, :]
        send[(c + 1) * p.S3 - 1 : (c + 1) * p.S3, :] = squares[0:1, :]


def out_kernel(p, recv, mean, log_share, mass_total, mean_out, loyalty_out):
    predicted = chunk_sum(p, recv, p.S3, p.i8) / mass_total[...]
    mean_out[...] = mean[...] + log_share[...] - jnp.log(predicted)
    squares = recv[p.S3 - 1 : p.S3, :]
    for c in range(1, p.C):
        squares = squares + recv[(c + 1) * p.S3 - 1 : (c + 1) * p.S3, :]
    clip = clip_of(p, squares)
    for t in range(p.R // LANES):
        values = []
        for b in range(p.hh):
            at = (t * p.hh + b) * p.S3 + p.i8
            values.append(recv[at : at + p.oi, :] + clip * recv[at + p.oi : at + 2 * p.oi, :])
        for o in range(p.hh):
            row = None
            for b in range(p.hh):
                shift = ((b - o) * p.RL) % LANES
                moved = pltpu.roll(values[b], shift, 1) if shift else values[b]
                row = moved if row is None else jnp.where(block_mask(p, p.oi, b), moved, row)
            loyalty_out[o * p.oi : (o + 1) * p.oi, t * LANES : (t + 1) * LANES] = row


def local(
    mean_utility,
    market_share,
    product_traits,
    taste_draws,
    taste_scale,
    type_weight,
    market_size,
    product_firm,
    firm_order,
    loyalty,
    firm_share,
):
    p = Plan(
        lax.axis_size(AXES),
        mean_utility.shape[0],
        mean_utility.shape[1],
        taste_scale.shape[0],
        firm_share.shape[1],
        firm_share.shape[0],
        loyalty.shape[0],
    )
    index = lax.axis_index(AXES)
    half, place = index % 2, index // 2

    def exchange(x):
        return lax.all_to_all(x, AXES, split_axis=0, concat_axis=0, tiled=True, axis_index_groups=p.groups)

    def swap(x):
        return lax.ppermute(x, AXES, p.swap)

    def kernel(fn, *args, **kwargs):
        return functools.partial(fn, p, *args, **kwargs)

    def packed_products(x):
        return x.reshape(p.h, p.i8, p.J).transpose(1, 0, 2).reshape(p.i8, LANES)

    mass = market_size[:, None] * type_weight
    mass_total = packed_products(jnp.broadcast_to(jnp.sum(mass, axis=1)[:, None], mean_utility.shape))
    log_share = packed_products(jnp.log(market_share))
    mean = packed_products(mean_utility)
    share = lax.dynamic_slice_in_dim(firm_share, place * p.RL, p.RL, axis=1)
    share = share.reshape(p.hh, p.FP, p.RL).transpose(1, 0, 2).reshape(p.FP, LANES)
    order = firm_order.reshape(p.C, 2, p.own)
    order = jnp.pad(order, ((0, 0), (0, 0), (0, p.ownp - p.own)), constant_values=-1)
    order = order.reshape(p.C, 2, p.hh, p.oi).transpose(1, 2, 0, 3).reshape(2, p.hh, p.OR)
    order_mine = lax.dynamic_index_in_dim(order, half, 0, keepdims=False)
    order_other = lax.dynamic_index_in_dim(order, 1 - half, 0, keepdims=False)
    order_rows = jnp.concatenate([order_mine, order_other], axis=0)
    order_columns = order_mine.T

    send = call(
        kernel(pack_kernel),
        sds((p.C * p.S, LANES)),
        (
            taste_draws.transpose(1, 0, 2),
            mass,
            product_traits.transpose(2, 0, 1) * taste_scale[:, None, None],
            product_firm.astype(F32),
            mean_utility,
            jnp.pad(loyalty, ((0, p.ownp - p.own), (0, 0))),
        ),
    )
    recv = exchange(send)
    taste, firms_t, mean_t, mass_t, mass_row, loy = call(
        kernel(prep_kernel),
        (
            sds((p.J, p.RL, p.ML)),
            sds((p.hh, p.J, LANES), jnp.int32),
            sds((p.hh, p.J, LANES)),
            sds((p.RL, p.ML)),
            sds((8, LANES)),
            sds((p.OR, LANES)),
        ),
        (recv,),
        scratch=(
            pltpu.VMEM((p.G, LANES), F32),
            pltpu.VMEM((p.K, p.RL, p.ML), F32),
            pltpu.VMEM((p.K, p.hh, p.J, LANES), F32),
        ),
    )
    table = call(kernel(table_kernel), sds((p.FP, LANES)), (loy, swap(loy), order_rows))

    def gather(packed):
        return call(
            kernel(gather_kernel),
            sds((p.J, p.RL, p.ML)),
            (packed, firms_t),
            scratch=(pltpu.VMEM((p.hh, 3 * p.RL, p.FP), BF),),
        )

    choice_outs = (
        sds((p.J, p.RL, p.ML)),
        sds((p.J, p.NR, p.ML), BF),
        sds((p.C * p.i8, LANES)),
    )
    choice_scratch = (pltpu.VMEM((p.J, p.RL, LANES), F32), pltpu.VMEM((p.hh, p.J, LANES), F32))
    found = gather(table)
    base, parts, pred = call(
        kernel(choice_first_kernel), choice_outs, (taste, found, mean_t, mass_t), scratch=choice_scratch, alias={0: 0}
    )
    gaps, clips = [], []
    for step in range(ITERS):
        last = step == ITERS - 1
        totals = call(
            kernel(scatter_kernel),
            sds((p.FP + 8, LANES)),
            (parts, firms_t, mass_row),
            scratch=(pltpu.VMEM((p.F, p.NR), F32),),
        )
        other = swap(totals)
        if last:
            break
        gap, squares = call(kernel(gap_kernel), (sds((p.FP, LANES)), sds((8, LANES))), (totals, other, share))
        gaps.append(gap)
        mean, send = call(
            kernel(mean_kernel),
            (sds((p.i8, LANES)), sds((p.C * p.S2, LANES))),
            (exchange(pred), mean, log_share, mass_total, squares),
        )
        recv = exchange(send)
        found = gather(gap)
        base, parts, pred, clip = call(
            kernel(choice_next_kernel),
            choice_outs + (sds((8, LANES)),),
            (base, found, recv, mass_t),
            scratch=choice_scratch + (pltpu.VMEM((p.G, LANES), F32),),
            alias={0: 0},
        )
        clips.append(clip)
    send = call(
        kernel(final_kernel),
        sds((p.C * p.S3, LANES)),
        (totals, other, share, table, gaps[0], gaps[1], jnp.concatenate(clips, axis=0), order_columns, pred),
    )
    mean_out, loyalty_out = call(
        kernel(out_kernel),
        (sds((p.i8, LANES)), sds((p.ownp, p.R))),
        (exchange(send), mean, log_share, mass_total),
    )
    mean_out = mean_out.reshape(p.i8, p.h, p.J).transpose(1, 0, 2).reshape(p.M, p.J)
    return (mean_out, loyalty_out[0 : p.own])


def solution(mesh):
    both = ("mkt", "grp")
    placed = (
        P(both, None),
        P(both, None),
        P(both, None, None),
        P(both, None, None),
        P(),
        P(both, None),
        P(both),
        P(both, None),
        P(),
        P(both, None),
        P(),
    )
    return jax.shard_map(
        local,
        mesh=mesh,
        in_specs=placed,
        out_specs=(P(both, None), P(both, None)),
        check_vma=False,
    )
```

```python
import functools

import jax
import jax.numpy as jnp
from jax import lax
from jax.experimental import pallas as pl
from jax.experimental.pallas import tpu as pltpu
from jax.sharding import PartitionSpec as P

ITERS = 3
LANES = 128
clip_target = 0.5
norm_eps = 1e-06
BF = jnp.bfloat16
F32 = jnp.float32


class Plan:
    def __init__(self, mkt, grp, own_markets, products, traits, types, firms, own_firms):
        self.C, self.Q = mkt, grp
        self.M, self.J, self.K = own_markets, products, traits
        self.R, self.F, self.own = types, firms, own_firms
        self.RL = types // mkt
        self.hh = LANES // self.RL
        self.ii = own_markets // self.hh
        self.h = LANES // products
        self.i8 = own_markets // self.h
        self.top = max(self.hh, self.h)
        self.w = own_markets // self.top
        self.ML = own_markets * mkt
        self.PR = mkt * self.i8
        self.FP = firms // self.hh
        self.HR = self.FP // 2
        self.ownp = -(-own_firms // self.hh) * self.hh
        self.oi = self.ownp // self.hh
        self.u = max(1, 256 // self.ML)
        self.NS = products // self.u
        self.NR = max(LANES, 2 * self.RL)
        self.s_draws = 0
        self.s_mass = self.s_draws + traits * self.ii
        self.s_loy = self.s_mass + self.ii
        self.s_traits = self.s_loy + self.oi
        self.s_firms = self.s_traits + traits * self.i8
        self.s_mean = self.s_firms + self.i8
        self.s_shift = self.s_mean + self.i8
        self.S = -(-(self.s_shift + self.i8) // 8) * 8
        self.PB = self.hh * products
        self.S2 = self.PB + 8
        self.S3 = -(-(self.i8 + 2 * self.oi + 1) // 8) * 8
        self.vmem = 16 if firms * products * self.ML <= 2**22 else 58


VM = pl.BlockSpec(memory_space=pltpu.VMEM)
SM = pl.BlockSpec(memory_space=pltpu.SMEM)
HBM = pl.BlockSpec(memory_space=pltpu.HBM)


def call(p, kernel, outs, args, scratch=(), specs=None, out_specs=None, flops=0):
    return pl.pallas_call(
        functools.partial(kernel, p),
        out_shape=outs,
        in_specs=specs or [VM] * len(args),
        out_specs=out_specs or jax.tree.map(lambda _: VM, outs),
        scratch_shapes=list(scratch),
        compiler_params=pltpu.CompilerParams(vmem_limit_bytes=p.vmem * 2**20),
    )(*args)


def sds(shape, dtype=F32):
    return jax.ShapeDtypeStruct(shape, dtype)


def block_mask(width, rows, b):
    return lax.broadcasted_iota(jnp.int32, (rows, LANES), 1) // width == b


def fold(p, x):
    total = x
    for b in range(1, p.hh):
        total = total + pltpu.roll(x, b * p.RL, 1)
    return total


def split2(x):
    a = x.astype(BF)
    return a, (x - a.astype(F32)).astype(BF)


def split3(x):
    a = x.astype(BF)
    b, c = split2(x - a.astype(F32))
    return a, b, c


def dot(a, b):
    return jnp.dot(a, b, preferred_element_type=F32)


def dot_t(a, b):
    return lax.dot_general(a, b, (((1,), (1,)), ((), ())), preferred_element_type=F32)


def moved(x, shift):
    return pltpu.roll(x, shift % LANES, 1) if shift % LANES else x


def pack_kernel(
    p, scale, size, draws_h, weight_h, loyalty_h, traits_h, firms_h, mean_h, share_h, out_h,
    draws, weight, loyalty, traits, firms, mean, share, out, sems, out_sems,
):
    pairs = (
        (draws_h, draws), (weight_h, weight), (traits_h, traits), (firms_h, firms),
        (mean_h, mean), (share_h, share), (loyalty_h, loyalty),
    )
    copies = [pltpu.make_async_copy(a, b, sems.at[n]) for n, (a, b) in enumerate(pairs)]
    for copy in copies:
        copy.start()
    for copy in copies:
        copy.wait()
    row = lax.broadcasted_iota(jnp.int32, (p.M, LANES), 0)
    column = jnp.zeros((p.M, LANES), F32)
    for m in range(p.M):
        column = jnp.where(row == m, size[m], column)
    mass_total = None
    tiles = []
    for t in range(p.R // LANES):
        tile = weight[:, t * LANES : (t + 1) * LANES] * column
        tiles.append(tile)
        mass_total = tile if mass_total is None else mass_total + tile
    mass_total = jnp.sum(mass_total, axis=1, keepdims=True)

    def by_type(tile_of, c, section, rows):
        tile, b = tile_of(c // p.hh), c % p.hh
        value = tile[0:rows, :] if not b else moved(tile, -b * p.RL)[0:rows, :]
        for q in range(1, p.hh):
            piece = moved(tile, (q - b) * p.RL)[q * rows : (q + 1) * rows, :]
            value = jnp.where(block_mask(p.RL, rows, q), piece, value)
        out[c * p.S + section : c * p.S + section + rows, :] = value

    def packed(x):
        return jnp.concatenate([x[q * p.i8 : (q + 1) * p.i8, :] for q in range(p.h)], axis=1)

    products = [packed(traits[k] * scale[k]) for k in range(p.K)]
    products += [packed(firms[...].astype(F32)), packed(mean[...])]
    products += [packed(jnp.log(share[...]) + jnp.log(mass_total))]
    sends = []
    for c in range(p.C):
        for k in range(p.K):
            by_type(lambda t: draws[k, :, t * LANES : (t + 1) * LANES], c, p.s_draws + k * p.ii, p.ii)
        by_type(lambda t: tiles[t], c, p.s_mass, p.ii)
        by_type(lambda t: loyalty[:, t * LANES : (t + 1) * LANES], c, p.s_loy, p.oi)
        for n, value in enumerate(products):
            at = c * p.S + p.s_traits + n * p.i8
            out[at : at + p.i8, :] = value
        part = pl.ds(c * p.S, p.S)
        copy = pltpu.make_async_copy(out.at[part], out_h.at[part], out_sems.at[c])
        copy.start()
        sends.append(copy)
    for copy in sends:
        copy.wait()


def prep_kernel(p, recv, firms_t, mean_t, shift_t, mass_t, mass_row, loy, draws_t, traits_t, nat):
    ta = p.top // p.hh

    def typed(section, store):
        for a in range(ta):
            for c in range(p.C):
                at = c * p.S + section + a * p.w
                nat[(a * p.C + c) * p.w : (a * p.C + c + 1) * p.w, :] = recv[at : at + p.w, :]
        flat = nat[0:LANES, :]
        turned = flat.T
        for b in range(p.hh):
            store(b, turned[b * p.RL : (b + 1) * p.RL, :])
        return flat

    def put_mass(b, value):
        mass_t[:, b * LANES : (b + 1) * LANES] = value

    flat = typed(p.s_mass, put_mass)
    row = jnp.sum(flat, axis=0, keepdims=True)
    mass_row[...] = fold(p, jnp.broadcast_to(row, (8, LANES)))
    for k in range(p.K):

        def put_draws(b, value):
            draws_t[k, :, b * LANES : (b + 1) * LANES] = value

        typed(p.s_draws + k * p.ii, put_draws)

    tb = p.top // p.h

    def product(section, store):
        for copy in range(max(1, LANES // p.PR)):
            for a in range(tb):
                for c in range(p.C):
                    at = c * p.S + section + a * p.w
                    to = copy * p.PR + (a * p.C + c) * p.w
                    nat[to : to + p.w, :] = recv[at : at + p.w, :]
        if p.PR >= LANES:
            per = p.PR // LANES
            for gi in range(per):
                turned = nat[gi * LANES : (gi + 1) * LANES, :].T
                for q in range(p.h):
                    store(q * per + gi, turned[q * p.J : (q + 1) * p.J, :])
        else:
            per = LANES // p.PR
            turned = nat[0:LANES, :].T
            for b in range(p.hh):
                value = turned[b * per * p.J : (b * per + 1) * p.J, :]
                for s in range(1, per):
                    at = (b * per + s) * p.J
                    value = jnp.where(block_mask(p.PR, p.J, s), turned[at : at + p.J, :], value)
                store(b, value)

    def into(ref):
        def store(b, value):
            ref[b] = value

        return store

    product(p.s_firms, into(firms_t))
    product(p.s_mean, into(mean_t))
    product(p.s_shift, into(shift_t))
    for k in range(p.K):
        product(p.s_traits + k * p.i8, into(traits_t.at[k]))
    loy[...] = jnp.zeros_like(loy)
    for c in range(p.C):
        loy[c * p.oi : (c + 1) * p.oi, :] = recv[c * p.S + p.s_loy : c * p.S + p.s_loy + p.oi, :]


def taste_kernel(p, draws_t, traits_t, firms_t, taste, hot):
    rows = min(p.F, 256)
    firm = lax.broadcasted_iota(jnp.int32, (rows, LANES), 0).astype(F32).astype(BF)

    def body(n, _):
        for v in range(p.u):
            j = n * p.u + v
            for b in range(p.hh):
                at = slice(b * LANES, (b + 1) * LANES)
                value = None
                for k in range(p.K):
                    term = traits_t[k, b, pl.ds(j, 1), :] * draws_t[k, :, at]
                    value = term if value is None else value + term
                taste[j, :, at] = value
                row = firms_t[b, pl.ds(j, 1), :]
                to = slice(v * p.ML + b * LANES, v * p.ML + (b + 1) * LANES)
                for base in range(0, p.F, rows):
                    want = jnp.broadcast_to(row - float(base), (rows, LANES)).astype(BF)
                    hot[n, base : base + rows, to] = jnp.where(firm == want, jnp.ones((), BF), jnp.zeros((), BF))
        return 0

    lax.fori_loop(0, p.NS, body, 0)


def table_kernel(p, place, order, share_h, *refs):
    blocks, (table, share, columns, tile, sem) = refs[:-5], refs[-5:]
    lane = place[0] * p.RL
    start = pl.multiple_of(lane // LANES * LANES, LANES)
    copy = pltpu.make_async_copy(share_h.at[:, pl.ds(start, LANES)], tile, sem)
    copy.start()
    firm = lax.broadcasted_iota(jnp.int32, (p.F, LANES), 0)
    total = jnp.zeros((p.F, LANES), F32)
    blocks = [ref[at : at + LANES, :] for ref in blocks for at in range(0, ref.shape[0], LANES)]
    for s, block in enumerate(blocks):
        pieces = jnp.concatenate(split3(block), axis=1)
        member = place[1] ^ s
        for b in range(p.hh):
            hot = (firm == order[pl.ds(member * p.hh + b, 1), :]).astype(F32).astype(BF)
            found = dot(hot, pieces)
            found = found[:, 0:LANES] + found[:, LANES : 2 * LANES] + found[:, 2 * LANES :]
            if p.hh > 1:
                found = jnp.where(block_mask(p.RL, p.F, b), found, 0.0)
            total = total + found
    pack_table(p, fold(p, total), table)
    for b in range(p.hh):
        row = order[pl.ds(place[1] * p.hh + b, 1), :].astype(F32)
        columns[b] = jnp.broadcast_to(row, (LANES, LANES)).T
    copy.wait()
    if p.hh == 1:
        share[...] = tile[...]
    else:
        for b in range(p.hh):
            part = pltpu.roll(tile[b * p.FP : (b + 1) * p.FP, :], (b * p.RL + LANES - (lane - start)) % LANES, 1)
            mask = block_mask(p.RL, p.FP, b)
            share[...] = part if not b else jnp.where(mask, part, share[...])


def pack_table(p, full, out):
    value = full[0 : p.FP, :]
    for b in range(1, p.hh):
        value = jnp.where(block_mask(p.RL, p.FP, b), full[b * p.FP : (b + 1) * p.FP, :], value)
    out[...] = value


def clip_of(p, squares):
    return jnp.minimum(1.0, clip_target / jnp.sqrt(squares / (p.F * p.R) + norm_eps))


def sum_chunks(p, recv, step, start, rows):
    total = recv[start : start + rows, :]
    for c in range(1, p.C):
        total = total + recv[c * step + start : c * step + start + rows, :]
    return total


def step_body(p, place, table, mean_of, taste, hot, mass_t, mass_row, pred, keep, give, tab, expu, parts, acc):
    turned = table[...].T
    for q, piece in enumerate(split2(turned)):
        for b in range(p.hh):
            tab[b, q * p.RL : (q + 1) * p.RL, :] = piece[b * p.RL : (b + 1) * p.RL, :]

    def gather(n, total):
        if p.hh == 1:
            found = dot(tab[0], hot[n])
        else:
            found = dot(tab[0], hot[n, 0 : p.FP, :])
            for b in range(1, p.hh):
                found = found + dot(tab[b], hot[n, b * p.FP : (b + 1) * p.FP, :])
        found = found[0 : p.RL] + found[p.RL : 2 * p.RL]
        for v in range(p.u):
            j = n * p.u + v
            means = [jnp.broadcast_to(mean_of[b, pl.ds(j, 1), :], (p.RL, LANES)) for b in range(p.hh)]
            means = means[0] if p.hh == 1 else jnp.concatenate(means, axis=1)
            e = jnp.exp(taste[j] + found[:, v * p.ML : (v + 1) * p.ML] + means)
            expu[j] = e
            total = total + e
        return total

    total = lax.fori_loop(0, p.NS, gather, jnp.zeros((p.RL, p.ML), F32), unroll=2)
    scale = mass_t[...] / (1.0 + total)
    acc[...] = jnp.zeros_like(acc)
    if p.NR > 2 * p.RL:
        parts[...] = jnp.zeros_like(parts)
    per = 2

    def scatter(n, _):
        value = None
        for s in range(per):
            for v in range(p.u):
                j = (n * per + s) * p.u + v
                x = expu[j] * scale
                hi, lo = split2(x)
                at = slice(v * p.ML, (v + 1) * p.ML)
                parts[s, 0 : p.RL, at] = hi
                parts[s, p.RL : 2 * p.RL, at] = lo
                row = jnp.sum(x, axis=0, keepdims=True)
                for b in range(p.hh):
                    pred[pl.ds(b * p.J + j, 1), :] = row[:, b * LANES : (b + 1) * LANES]
            term = dot_t(hot[n * per + s], parts[s])
            value = term if value is None else value + term
        acc[...] += value
        return 0

    lax.fori_loop(0, p.NS // per, scatter, 0)
    full = acc[:, 0:LANES]
    for t in range(1, p.NR // LANES):
        full = full + acc[:, t * LANES : (t + 1) * LANES]
    if p.hh == 1:
        acc[:, 0:LANES] = full
    else:
        pack_table(p, fold(p, full), acc.at[0 : p.FP, 0:LANES])
    mine = (place[1] & 1) * p.HR
    keep[0 : p.HR, :] = acc[pl.ds(pl.multiple_of(mine, 8), p.HR), 0:LANES]
    give[0 : p.HR, :] = acc[pl.ds(pl.multiple_of(p.HR - mine, 8), p.HR), 0:LANES]
    keep[p.HR :, :] = mass_row[...]
    give[p.HR :, :] = mass_row[...]


def first_kernel(p, place, table, mean_t, taste, hot, mass_t, mass_row, pred, keep, give, *scratch):
    step_body(p, place, table, mean_t, taste, hot, mass_t, mass_row, pred, keep, give, *scratch)


def next_kernel(
    p, place, recv, gap_mine, gap_other, table_in, mean_in, shift_t, taste, hot, mass_t, mass_row,
    table, mean_t, pred, keep, give, *scratch
):
    clip = clip_of(p, sum_chunks(p, recv, p.S2, p.PB, 1))
    mine = (place[1] & 1) * p.HR
    for ref, start in ((gap_mine, mine), (gap_other, p.HR - mine)):
        at = pl.ds(pl.multiple_of(start, 8), p.HR)
        table[at, :] = table_in[at, :] + clip * ref[0 : p.HR, :]
    for b in range(p.hh):
        total = sum_chunks(p, recv, p.S2, b * p.J, p.J)
        mean_t[b] = mean_in[b] + shift_t[b] - jnp.log(total)
    step_body(p, place, table, mean_t, taste, hot, mass_t, mass_row, pred, keep, give, *scratch)


def add_kernel(p, a, b, out):
    out[...] = a[...] + b[...]


def gap_kernel(p, place, mine, other, share, gap):
    total = mine[...] + other[...]
    at = pl.ds(pl.multiple_of((place[1] & 1) * p.HR, 8), p.HR)
    value = jnp.log(share[at, :]) - jnp.log(total[0 : p.HR, :] / total[p.HR : p.HR + 1, :])
    gap[0 : p.HR, :] = value
    rows = jnp.sum(value * value, axis=0, keepdims=True)
    gap[p.HR :, :] = jnp.broadcast_to(jnp.sum(rows, axis=1, keepdims=True), (8, LANES))


def send_kernel(p, gap_mine, gap_other, pred, send):
    squares = gap_mine[p.HR :, :] + gap_other[p.HR :, :]
    value = pred[...]
    for c in range(p.C):
        send[c * p.S2 : c * p.S2 + p.PB, :] = value
        send[c * p.S2 + p.PB : (c + 1) * p.S2, :] = squares


def final_kernel(p, place, gap_mine, gap_other, table, columns, pred, mean_t, shift_t, send, own, gap, nat, means):
    mine = (place[1] & 1) * p.HR
    for ref, start in ((gap_mine, mine), (gap_other, p.HR - mine)):
        gap[pl.ds(pl.multiple_of(start, 8), p.HR), :] = ref[0 : p.HR, :]
    squares = gap_mine[p.HR : p.HR + 1, :] + gap_other[p.HR : p.HR + 1, :]
    lane = lax.broadcasted_iota(jnp.int32, (LANES, LANES), 1).astype(F32)
    for n, ref in enumerate((table, gap)):
        pieces = jnp.concatenate(split3(ref[...]), axis=1)
        picked = None
        for o in range(p.hh):
            total = None
            for b in range(p.hh):
                wide = -(-p.FP // LANES)
                hot = [columns[o] == lane + float(b * p.FP + t * LANES) for t in range(wide)]
                hot = jnp.concatenate([x.astype(F32).astype(BF) for x in hot], axis=1)[:, 0 : p.FP]
                found = dot(hot, pieces)
                found = found[:, 0:LANES] + found[:, LANES : 2 * LANES] + found[:, 2 * LANES :]
                if p.hh > 1:
                    found = jnp.where(block_mask(p.RL, LANES, b), found, 0.0)
                total = found if total is None else total + found
            total = fold(p, total)
            picked = total if picked is None else jnp.where(block_mask(p.RL, LANES, o), total, picked)
        at = p.i8 + n * p.oi
        for c in range(p.C):
            send[c * p.S3 + at : c * p.S3 + at + p.oi, :] = picked[c * p.oi : (c + 1) * p.oi, :]
    tb = p.top // p.h

    def by_owner(block, store):
        if p.PR >= LANES:
            per = p.PR // LANES
            for gi in range(per):
                tall = [block(q * per + gi) for q in range(p.h)]
                nat[gi * LANES : (gi + 1) * LANES, :] = jnp.concatenate(tall, axis=0).T
        else:
            per = LANES // p.PR
            tall = [moved(block(q // per), -(q % per) * p.PR) for q in range(p.h)]
            nat[0:LANES, :] = jnp.concatenate(tall, axis=0).T
        for c in range(p.C):
            for a in range(tb):
                at = (a * p.C + c) * p.w
                store(c, slice(a * p.w, (a + 1) * p.w), nat[at : at + p.w, :])

    def put_mean(c, at, value):
        means[c, at, :] = value

    def put_pred(c, at, value):
        send[c * p.S3 + at.start : c * p.S3 + at.stop, :] = value

    by_owner(lambda b: mean_t[b] + shift_t[b], put_mean)
    by_owner(lambda b: pred[b * p.J : (b + 1) * p.J, :], put_pred)
    own[...] = means[place[0]]
    for c in range(p.C):
        send[(c + 1) * p.S3 - 1 : (c + 1) * p.S3, :] = squares


def out_kernel(p, recv, own, mean_out, loyalty_out):
    predicted = sum_chunks(p, recv, p.S3, 0, p.i8)
    value = own[...] - jnp.log(predicted)
    for q in range(p.h):
        mean_out[q * p.i8 : (q + 1) * p.i8, :] = moved(value, -q * p.J)[:, 0 : p.J]
    clip = clip_of(p, sum_chunks(p, recv, p.S3, p.S3 - 1, 1))
    for t in range(p.R // LANES):
        values = []
        for b in range(p.hh):
            at = (t * p.hh + b) * p.S3 + p.i8
            values.append(recv[at : at + p.oi, :] + clip * recv[at + p.oi : at + 2 * p.oi, :])
        for o in range(p.hh):
            row = moved(values[0], -o * p.RL)
            for b in range(1, p.hh):
                row = jnp.where(block_mask(p.RL, p.oi, b), moved(values[b], (b - o) * p.RL), row)
            loyalty_out[o * p.oi : (o + 1) * p.oi, t * LANES : (t + 1) * LANES] = row


def local(
    mean_utility,
    market_share,
    product_traits,
    taste_draws,
    taste_scale,
    type_weight,
    market_size,
    product_firm,
    firm_order,
    loyalty,
    firm_share,
):
    p = Plan(
        lax.axis_size("mkt"),
        lax.axis_size("grp"),
        mean_utility.shape[0],
        mean_utility.shape[1],
        taste_scale.shape[0],
        firm_share.shape[1],
        firm_share.shape[0],
        loyalty.shape[0],
    )
    place = jnp.stack([lax.axis_index("mkt"), lax.axis_index("grp")]).astype(jnp.int32)

    def exchange(x):
        return lax.all_to_all(x, "mkt", split_axis=0, concat_axis=0, tiled=True)

    def swap(x, bit):
        return lax.ppermute(x, "grp", [(q, q ^ bit) for q in range(p.Q)])

    order = firm_order.reshape(p.C, p.Q, p.own)
    order = jnp.pad(order, ((0, 0), (0, 0), (0, p.ownp - p.own)), constant_values=-1)
    order = order.reshape(p.C, p.Q, p.hh, p.oi).transpose(1, 2, 0, 3).reshape(p.Q * p.hh, p.C * p.oi)
    order = jnp.pad(order, ((0, 0), (0, LANES - p.C * p.oi)), constant_values=-1)
    if p.ownp > p.own:
        loyalty = jnp.pad(loyalty, ((0, p.ownp - p.own), (0, 0)))

    send = call(
        p,
        pack_kernel,
        sds((p.C * p.S, LANES)),
        (
            taste_scale,
            market_size,
            taste_draws.transpose(1, 0, 2),
            type_weight,
            loyalty,
            product_traits.transpose(2, 0, 1),
            product_firm,
            mean_utility,
            market_share,
        ),
        specs=[SM, SM] + [HBM] * 7,
        out_specs=HBM,
        scratch=(
            pltpu.VMEM((p.K, p.M, p.R), F32),
            pltpu.VMEM((p.M, p.R), F32),
            pltpu.VMEM((p.ownp, p.R), F32),
            pltpu.VMEM((p.K, p.M, p.J), F32),
            pltpu.VMEM((p.M, p.J), jnp.int32),
            pltpu.VMEM((p.M, p.J), F32),
            pltpu.VMEM((p.M, p.J), F32),
            pltpu.VMEM((p.C * p.S, LANES), F32),
            pltpu.SemaphoreType.DMA((7,)),
            pltpu.SemaphoreType.DMA((p.C,)),
        ),
    )
    tiles = sds((p.hh, p.J, LANES))
    firms_t, mean_t, shift_t, mass_t, mass_row, loy, draws_t, traits_t = call(
        p,
        prep_kernel,
        (
            tiles,
            tiles,
            tiles,
            sds((p.RL, p.ML)),
            sds((8, LANES)),
            sds((LANES, LANES)),
            sds((p.K, p.RL, p.ML)),
            sds((p.K, p.hh, p.J, LANES)),
        ),
        (exchange(send),),
        scratch=(pltpu.VMEM((max(LANES, p.PR), LANES), F32),),
    )
    rows = [loy]
    bit = 1
    while bit < p.Q:
        rows.append(swap(rows[0] if bit == 1 else jnp.concatenate(rows, axis=0), bit))
        bit *= 2
    taste, hot = call(
        p,
        taste_kernel,
        (sds((p.J, p.RL, p.ML)), sds((p.NS, p.F, p.u * p.ML), BF)),
        (draws_t, traits_t, firms_t),
    )
    table, share, columns = call(
        p,
        table_kernel,
        (sds((p.FP, LANES)), sds((p.FP, LANES)), sds((p.hh, LANES, LANES))),
        (place, order, firm_share, *rows),
        specs=[SM, VM, HBM] + [VM] * len(rows),
        scratch=(pltpu.VMEM((p.F, LANES), F32), pltpu.SemaphoreType.DMA(())),
    )
    half = sds((p.HR + 8, LANES))
    step_outs = (sds((p.PB, LANES)), half, half)
    step_scratch = (
        pltpu.VMEM((p.hh, 2 * p.RL, p.FP), BF),
        pltpu.VMEM((p.J, p.RL, p.ML), F32),
        pltpu.VMEM((2, p.NR, p.u * p.ML), BF),
        pltpu.VMEM((p.F, p.NR), F32),
    )
    fixed = (taste, hot, mass_t, mass_row)
    for step in range(ITERS):
        if step == 0:
            pred, keep, give = call(
                p,
                first_kernel,
                step_outs,
                (place, table, mean_t, *fixed),
                specs=[SM] + [VM] * 6,
                scratch=step_scratch,
            )
        else:
            table, mean_t, pred, keep, give = call(
                p,
                next_kernel,
                (sds((p.FP, LANES)), tiles) + step_outs,
                (place, recv, gap_mine, gap_other, table, mean_t, shift_t, *fixed),
                specs=[SM] + [VM] * 10,
                scratch=step_scratch,
            )
        mine = call(p, add_kernel, half, (keep, swap(give, 1)))
        bit = 2
        while 2 * bit < p.Q:
            mine = call(p, add_kernel, half, (mine, swap(mine, bit)))
            bit *= 2
        gap_mine = call(p, gap_kernel, half, (place, mine, swap(mine, bit), share), specs=[SM, VM, VM, VM])
        gap_other = swap(gap_mine, 1)
        if step < ITERS - 1:
            recv = exchange(call(p, send_kernel, sds((p.C * p.S2, LANES)), (gap_mine, gap_other, pred)))
    send, own = call(
        p,
        final_kernel,
        (sds((p.C * p.S3, LANES)), sds((p.i8, LANES))),
        (place, gap_mine, gap_other, table, columns, pred, mean_t, shift_t),
        specs=[SM] + [VM] * 7,
        scratch=(
            pltpu.VMEM((p.FP, LANES), F32),
            pltpu.VMEM((max(LANES, p.PR), LANES), F32),
            pltpu.VMEM((p.C, p.i8, LANES), F32),
        ),
    )
    mean_out, loyalty_out = call(
        p, out_kernel, (sds((p.M, p.J)), sds((p.ownp, p.R))), (exchange(send), own)
    )
    return (mean_out, loyalty_out[0 : p.own] if p.ownp > p.own else loyalty_out)


def solution(mesh):
    both = ("mkt", "grp")
    placed = (
        P(both, None),
        P(both, None),
        P(both, None, None),
        P(both, None, None),
        P(),
        P(both, None),
        P(both),
        P(both, None),
        P(),
        P(both, None),
        P(),
    )
    return jax.shard_map(
        local,
        mesh=mesh,
        in_specs=placed,
        out_specs=(P(both, None), P(both, None)),
        check_vma=False,
    )
```

```python
import functools

import jax
import jax.numpy as jnp
from jax import lax
from jax.experimental import pallas as pl
from jax.experimental.pallas import tpu as pltpu
from jax.sharding import PartitionSpec as P

ITERS = 3
LANES = 128
clip_target = 0.5
norm_eps = 1e-06
BF = jnp.bfloat16
F32 = jnp.float32


class Plan:
    def __init__(self, mkt, grp, own_markets, products, traits, types, firms, own_firms):
        self.C, self.Q = mkt, grp
        self.M, self.J, self.K = own_markets, products, traits
        self.R, self.F, self.own = types, firms, own_firms
        self.RL = types // mkt
        self.hh = LANES // self.RL
        self.ii = own_markets // self.hh
        self.h = LANES // products
        self.i8 = own_markets // self.h
        self.top = max(self.hh, self.h)
        self.w = own_markets // self.top
        self.ML = own_markets * mkt
        self.PR = mkt * self.i8
        self.FP = firms // self.hh
        self.HR = self.FP // 2
        self.ownp = -(-own_firms // self.hh) * self.hh
        self.oi = self.ownp // self.hh
        self.u = max(1, 256 // self.ML)
        self.NS = products // self.u
        self.per = min(16, self.NS)
        self.NR = max(LANES, 2 * self.RL)
        self.s_draws = 0
        self.s_mass = self.s_draws + traits * self.ii
        self.s_loy = self.s_mass + self.ii
        self.s_traits = self.s_loy + self.oi
        self.s_firms = self.s_traits + traits * self.i8
        self.s_mean = self.s_firms + self.i8
        self.s_shift = self.s_mean + self.i8
        self.S = -(-(self.s_shift + self.i8) // 8) * 8
        self.PB = self.hh * products
        self.S2 = self.PB + 8
        self.S3 = -(-(self.i8 + 2 * self.oi + 1) // 8) * 8
        self.vmem = 16 if firms * products * self.ML <= 2**22 else 58


VM = pl.BlockSpec(memory_space=pltpu.VMEM)
SM = pl.BlockSpec(memory_space=pltpu.SMEM)
HBM = pl.BlockSpec(memory_space=pltpu.HBM)


def call(p, kernel, outs, args, scratch=(), specs=None, out_specs=None, vmem=None):
    return pl.pallas_call(
        functools.partial(kernel, p),
        out_shape=outs,
        in_specs=specs or [VM] * len(args),
        out_specs=out_specs or jax.tree.map(lambda _: VM, outs),
        scratch_shapes=list(scratch),
        compiler_params=pltpu.CompilerParams(vmem_limit_bytes=(vmem or p.vmem) * 2**20),
    )(*args)


def sds(shape, dtype=F32):
    return jax.ShapeDtypeStruct(shape, dtype)


def block_mask(width, rows, b):
    return lax.broadcasted_iota(jnp.int32, (rows, LANES), 1) // width == b


def fold(p, x):
    total = x
    for b in range(1, p.hh):
        total = total + pltpu.roll(x, b * p.RL, 1)
    return total


def split2(x):
    a = x.astype(BF)
    return a, (x - a.astype(F32)).astype(BF)


def split3(x):
    a = x.astype(BF)
    b, c = split2(x - a.astype(F32))
    return a, b, c


def dot(a, b):
    return jnp.dot(a, b, preferred_element_type=F32)


def dot_t(a, b):
    return lax.dot_general(a, b, (((1,), (1,)), ((), ())), preferred_element_type=F32)


def moved(x, shift):
    return pltpu.roll(x, shift % LANES, 1) if shift % LANES else x


def pack_kernel(
    p, scale, size, draws_h, weight_h, loyalty_h, traits_h, firms_h, mean_h, share_h, out_h,
    draws, weight, loyalty, traits, firms, mean, share, out, sems, out_sems,
):
    pairs = (
        (draws_h, draws), (weight_h, weight), (traits_h, traits), (firms_h, firms),
        (mean_h, mean), (share_h, share), (loyalty_h, loyalty),
    )
    copies = [pltpu.make_async_copy(a, b, sems.at[n]) for n, (a, b) in enumerate(pairs)]
    for copy in copies:
        copy.start()
    for copy in copies:
        copy.wait()
    row = lax.broadcasted_iota(jnp.int32, (p.M, LANES), 0)
    column = jnp.zeros((p.M, LANES), F32)
    for m in range(p.M):
        column = jnp.where(row == m, size[m], column)
    mass_total = None
    tiles = []
    for t in range(p.R // LANES):
        tile = weight[:, t * LANES : (t + 1) * LANES] * column
        tiles.append(tile)
        mass_total = tile if mass_total is None else mass_total + tile
    mass_total = jnp.sum(mass_total, axis=1, keepdims=True)

    def by_type(tile_of, c, section, rows):
        tile, b = tile_of(c // p.hh), c % p.hh
        value = tile[0:rows, :] if not b else moved(tile, -b * p.RL)[0:rows, :]
        for q in range(1, p.hh):
            piece = moved(tile, (q - b) * p.RL)[q * rows : (q + 1) * rows, :]
            value = jnp.where(block_mask(p.RL, rows, q), piece, value)
        out[c * p.S + section : c * p.S + section + rows, :] = value

    def packed(x):
        return jnp.concatenate([x[q * p.i8 : (q + 1) * p.i8, :] for q in range(p.h)], axis=1)

    products = [packed(traits[k] * scale[k]) for k in range(p.K)]
    products += [packed(firms[...].astype(F32)), packed(mean[...])]
    products += [packed(jnp.log(share[...]) + jnp.log(mass_total))]
    sends = []
    for c in range(p.C):
        for k in range(p.K):
            by_type(lambda t: draws[k, :, t * LANES : (t + 1) * LANES], c, p.s_draws + k * p.ii, p.ii)
        by_type(lambda t: tiles[t], c, p.s_mass, p.ii)
        by_type(lambda t: loyalty[:, t * LANES : (t + 1) * LANES], c, p.s_loy, p.oi)
        for n, value in enumerate(products):
            at = c * p.S + p.s_traits + n * p.i8
            out[at : at + p.i8, :] = value
        part = pl.ds(c * p.S, p.S)
        copy = pltpu.make_async_copy(out.at[part], out_h.at[part], out_sems.at[c])
        copy.start()
        sends.append(copy)
    for copy in sends:
        copy.wait()


def prep_kernel(p, recv, firms_t, mean_t, shift_t, mass_t, mass_row, loy, draws_t, traits_t, nat):
    ta = p.top // p.hh

    def typed(section, store):
        for a in range(ta):
            for c in range(p.C):
                at = c * p.S + section + a * p.w
                nat[(a * p.C + c) * p.w : (a * p.C + c + 1) * p.w, :] = recv[at : at + p.w, :]
        flat = nat[0:LANES, :]
        turned = flat.T
        for b in range(p.hh):
            store(b, turned[b * p.RL : (b + 1) * p.RL, :])
        return flat

    def put_mass(b, value):
        mass_t[:, b * LANES : (b + 1) * LANES] = value

    flat = typed(p.s_mass, put_mass)
    row = jnp.sum(flat, axis=0, keepdims=True)
    mass_row[...] = fold(p, jnp.broadcast_to(row, (8, LANES)))
    for k in range(p.K):

        def put_draws(b, value):
            draws_t[k, :, b * LANES : (b + 1) * LANES] = value

        typed(p.s_draws + k * p.ii, put_draws)

    tb = p.top // p.h

    def product(section, store):
        for copy in range(max(1, LANES // p.PR)):
            for a in range(tb):
                for c in range(p.C):
                    at = c * p.S + section + a * p.w
                    to = copy * p.PR + (a * p.C + c) * p.w
                    nat[to : to + p.w, :] = recv[at : at + p.w, :]
        if p.PR >= LANES:
            per = p.PR // LANES
            for gi in range(per):
                turned = nat[gi * LANES : (gi + 1) * LANES, :].T
                for q in range(p.h):
                    store(q * per + gi, turned[q * p.J : (q + 1) * p.J, :])
        else:
            per = LANES // p.PR
            turned = nat[0:LANES, :].T
            for b in range(p.hh):
                value = turned[b * per * p.J : (b * per + 1) * p.J, :]
                for s in range(1, per):
                    at = (b * per + s) * p.J
                    value = jnp.where(block_mask(p.PR, p.J, s), turned[at : at + p.J, :], value)
                store(b, value)

    def into(ref):
        def store(b, value):
            ref[b] = value

        return store

    product(p.s_firms, into(firms_t))
    product(p.s_mean, into(mean_t))
    product(p.s_shift, into(shift_t))
    for k in range(p.K):
        product(p.s_traits + k * p.i8, into(traits_t.at[k]))
    loy[...] = jnp.zeros_like(loy)
    for c in range(p.C):
        loy[c * p.oi : (c + 1) * p.oi, :] = recv[c * p.S + p.s_loy : c * p.S + p.s_loy + p.oi, :]


def taste_kernel(p, draws_t, traits_t, firms_t, taste, hot):
    rows = min(p.F, 256)
    firm = lax.broadcasted_iota(jnp.int32, (rows, LANES), 0).astype(F32).astype(BF)

    def body(n, _):
        for v in range(p.u):
            j = n * p.u + v
            for b in range(p.hh):
                at = slice(b * LANES, (b + 1) * LANES)
                value = None
                for k in range(p.K):
                    term = traits_t[k, b, pl.ds(j, 1), :] * draws_t[k, :, at]
                    value = term if value is None else value + term
                taste[j, :, at] = value
                row = firms_t[b, pl.ds(j, 1), :]
                for base in range(0, p.F, rows):
                    want = jnp.broadcast_to(row - float(base), (rows, LANES)).astype(BF)
                    hot[j, b, base : base + rows, :] = jnp.where(firm == want, jnp.ones((), BF), jnp.zeros((), BF))
        return 0

    lax.fori_loop(0, p.NS, body, 0)


def table_kernel(p, order, share_h, *refs):
    blocks, (table, share, columns, tile, sem) = refs[:-5], refs[-5:]
    lane = lax.axis_index("mkt") * p.RL
    start = pl.multiple_of(lane // LANES * LANES, LANES)
    copy = pltpu.make_async_copy(share_h.at[:, pl.ds(start, LANES)], tile, sem)
    copy.start()
    firm = lax.broadcasted_iota(jnp.int32, (p.F, LANES), 0)
    total = jnp.zeros((p.F, LANES), F32)
    blocks = [ref[at : at + LANES, :] for ref in blocks for at in range(0, ref.shape[0], LANES)]
    for s, block in enumerate(blocks):
        pieces = jnp.concatenate(split3(block), axis=1)
        member = lax.axis_index("grp") ^ s
        for b in range(p.hh):
            hot = (firm == order[pl.ds(member * p.hh + b, 1), :]).astype(F32).astype(BF)
            found = dot(hot, pieces)
            found = found[:, 0:LANES] + found[:, LANES : 2 * LANES] + found[:, 2 * LANES :]
            if p.hh > 1:
                found = jnp.where(block_mask(p.RL, p.F, b), found, 0.0)
            total = total + found
    pack_table(p, fold(p, total), table)
    for b in range(p.hh):
        row = order[pl.ds(lax.axis_index("grp") * p.hh + b, 1), :].astype(F32)
        columns[b] = jnp.broadcast_to(row, (LANES, LANES)).T
    copy.wait()
    if p.hh == 1:
        share[...] = tile[...]
    else:
        for b in range(p.hh):
            part = pltpu.roll(tile[b * p.FP : (b + 1) * p.FP, :], (b * p.RL + LANES - (lane - start)) % LANES, 1)
            mask = block_mask(p.RL, p.FP, b)
            share[...] = part if not b else jnp.where(mask, part, share[...])


def pack_table(p, full, out):
    value = full[0 : p.FP, :]
    for b in range(1, p.hh):
        value = jnp.where(block_mask(p.RL, p.FP, b), full[b * p.FP : (b + 1) * p.FP, :], value)
    out[...] = value


def clip_of(p, squares):
    return jnp.minimum(1.0, clip_target / jnp.sqrt(squares / (p.F * p.R) + norm_eps))


def sum_chunks(p, recv, step, start, rows):
    total = recv[start : start + rows, :]
    for c in range(1, p.C):
        total = total + recv[c * step + start : c * step + start + rows, :]
    return total


def step_body(p, table, mean_of, taste, hot, mass_t, mass_row, pred, keep, give, tab, expu, parts, acc):
    turned = table[...].T
    for q, piece in enumerate(split2(turned)):
        for t in range(p.F // LANES):
            b, at = divmod(t * LANES, p.FP)
            tab[t, q * p.RL : (q + 1) * p.RL, :] = piece[b * p.RL : (b + 1) * p.RL, at : at + LANES]

    def hot_of(n):
        return jnp.concatenate([hot[n * p.u + v, b] for v in range(p.u) for b in range(p.hh)], axis=1)

    def gather(n, total):
        found = dot(jnp.concatenate([tab[t] for t in range(p.F // LANES)], axis=1), hot_of(n))
        found = found[0 : p.RL] + found[p.RL : 2 * p.RL]
        for v in range(p.u):
            j = n * p.u + v
            means = [jnp.broadcast_to(mean_of[b, pl.ds(j, 1), :], (p.RL, LANES)) for b in range(p.hh)]
            means = means[0] if p.hh == 1 else jnp.concatenate(means, axis=1)
            e = jnp.exp(taste[j] + found[:, v * p.ML : (v + 1) * p.ML] + means)
            expu[j] = e
            total = total + e
        return total

    total = lax.fori_loop(0, p.NS, gather, jnp.zeros((p.RL, p.ML), F32), unroll=min(16, p.NS))
    scale = mass_t[...] / (1.0 + total)
    acc[...] = jnp.zeros_like(acc)
    if p.NR > 2 * p.RL:
        parts[...] = jnp.zeros_like(parts)
    per = p.per

    def scatter(n, _):
        value = None
        for s in range(per):
            for v in range(p.u):
                j = (n * per + s) * p.u + v
                x = expu[j] * scale
                hi, lo = split2(x)
                for b in range(p.hh):
                    at = slice(b * LANES, (b + 1) * LANES)
                    parts[s, v * p.hh + b, 0 : p.RL, :] = hi[:, at]
                    parts[s, v * p.hh + b, p.RL : 2 * p.RL, :] = lo[:, at]
                row = jnp.sum(x, axis=0, keepdims=True)
                for b in range(p.hh):
                    pred[pl.ds(b * p.J + j, 1), :] = row[:, b * LANES : (b + 1) * LANES]
            right = jnp.concatenate([parts[s, t] for t in range(p.u * p.hh)], axis=1)
            term = dot_t(hot_of(n * per + s), right)
            value = term if value is None else value + term
        acc[...] += value
        return 0

    lax.fori_loop(0, p.NS // per, scatter, 0)
    full = acc[:, 0:LANES]
    for t in range(1, p.NR // LANES):
        full = full + acc[:, t * LANES : (t + 1) * LANES]
    if p.hh == 1:
        acc[:, 0:LANES] = full
    else:
        pack_table(p, fold(p, full), acc.at[0 : p.FP, 0:LANES])
    mine = (lax.axis_index("grp") & 1) * p.HR
    keep[0 : p.HR, :] = acc[pl.ds(pl.multiple_of(mine, 8), p.HR), 0:LANES]
    give[0 : p.HR, :] = acc[pl.ds(pl.multiple_of(p.HR - mine, 8), p.HR), 0:LANES]
    keep[p.HR :, :] = mass_row[...]
    give[p.HR :, :] = mass_row[...]


def step_scratch_of(p):
    return (
        pltpu.VMEM((p.F // LANES, 2 * p.RL, LANES), BF),
        pltpu.VMEM((p.J, p.RL, p.ML), F32),
        pltpu.VMEM((p.per, p.u * p.hh, p.NR, LANES), BF),
        pltpu.VMEM((p.F, p.NR), F32),
    )


def first_kernel(p, table, mean_t, taste, hot, mass_t, mass_row, pred, keep, give, *scratch):
    step_body(p, table, mean_t, taste, hot, mass_t, mass_row, pred, keep, give, *scratch)


def next_kernel(
    p, recv, gap_mine, gap_other, table_in, mean_in, shift_t, taste, hot, mass_t, mass_row,
    table, mean_t, pred, keep, give, *scratch
):
    clip = clip_of(p, sum_chunks(p, recv, p.S2, p.PB, 1))
    mine = (lax.axis_index("grp") & 1) * p.HR
    for ref, start in ((gap_mine, mine), (gap_other, p.HR - mine)):
        at = pl.ds(pl.multiple_of(start, 8), p.HR)
        table[at, :] = table_in[at, :] + clip * ref[0 : p.HR, :]
    for b in range(p.hh):
        total = sum_chunks(p, recv, p.S2, b * p.J, p.J)
        mean_t[b] = mean_in[b] + shift_t[b] - jnp.log(total)
    step_body(p, table, mean_t, taste, hot, mass_t, mass_row, pred, keep, give, *scratch)


def add_kernel(p, a, b, out):
    out[...] = a[...] + b[...]


def gap_kernel(p, mine, other, share, gap):
    total = mine[...] + other[...]
    at = pl.ds(pl.multiple_of((lax.axis_index("grp") & 1) * p.HR, 8), p.HR)
    value = jnp.log(share[at, :]) - jnp.log(total[0 : p.HR, :] / total[p.HR : p.HR + 1, :])
    gap[0 : p.HR, :] = value
    rows = jnp.sum(value * value, axis=0, keepdims=True)
    gap[p.HR :, :] = jnp.broadcast_to(jnp.sum(rows, axis=1, keepdims=True), (8, LANES))


def send_kernel(p, gap_mine, gap_other, pred, send):
    squares = gap_mine[p.HR :, :] + gap_other[p.HR :, :]
    value = pred[...]
    for c in range(p.C):
        send[c * p.S2 : c * p.S2 + p.PB, :] = value
        send[c * p.S2 + p.PB : (c + 1) * p.S2, :] = squares


def final_kernel(p, gap_mine, gap_other, table, columns, pred, mean_t, shift_t, send, own, gap, nat, means):
    mine = (lax.axis_index("grp") & 1) * p.HR
    for ref, start in ((gap_mine, mine), (gap_other, p.HR - mine)):
        gap[pl.ds(pl.multiple_of(start, 8), p.HR), :] = ref[0 : p.HR, :]
    squares = gap_mine[p.HR : p.HR + 1, :] + gap_other[p.HR : p.HR + 1, :]
    lane = lax.broadcasted_iota(jnp.int32, (LANES, LANES), 1).astype(F32)
    for n, ref in enumerate((table, gap)):
        pieces = jnp.concatenate(split3(ref[...]), axis=1)
        picked = None
        for o in range(p.hh):
            total = None
            for b in range(p.hh):
                wide = -(-p.FP // LANES)
                hot = [columns[o] == lane + float(b * p.FP + t * LANES) for t in range(wide)]
                hot = jnp.concatenate([x.astype(F32).astype(BF) for x in hot], axis=1)[:, 0 : p.FP]
                found = dot(hot, pieces)
                found = found[:, 0:LANES] + found[:, LANES : 2 * LANES] + found[:, 2 * LANES :]
                if p.hh > 1:
                    found = jnp.where(block_mask(p.RL, LANES, b), found, 0.0)
                total = found if total is None else total + found
            total = fold(p, total)
            picked = total if picked is None else jnp.where(block_mask(p.RL, LANES, o), total, picked)
        at = p.i8 + n * p.oi
        for c in range(p.C):
            send[c * p.S3 + at : c * p.S3 + at + p.oi, :] = picked[c * p.oi : (c + 1) * p.oi, :]
    tb = p.top // p.h

    def by_owner(block, store):
        if p.PR >= LANES:
            per = p.PR // LANES
            for gi in range(per):
                tall = [block(q * per + gi) for q in range(p.h)]
                nat[gi * LANES : (gi + 1) * LANES, :] = jnp.concatenate(tall, axis=0).T
        else:
            per = LANES // p.PR
            tall = [moved(block(q // per), -(q % per) * p.PR) for q in range(p.h)]
            nat[0:LANES, :] = jnp.concatenate(tall, axis=0).T
        for c in range(p.C):
            for a in range(tb):
                at = (a * p.C + c) * p.w
                store(c, slice(a * p.w, (a + 1) * p.w), nat[at : at + p.w, :])

    def put_mean(c, at, value):
        means[c, at, :] = value

    def put_pred(c, at, value):
        send[c * p.S3 + at.start : c * p.S3 + at.stop, :] = value

    by_owner(lambda b: mean_t[b] + shift_t[b], put_mean)
    by_owner(lambda b: pred[b * p.J : (b + 1) * p.J, :], put_pred)
    own[...] = means[lax.axis_index("mkt")]
    for c in range(p.C):
        send[(c + 1) * p.S3 - 1 : (c + 1) * p.S3, :] = squares


def out_kernel(p, recv, own, mean_out, loyalty_out):
    predicted = sum_chunks(p, recv, p.S3, 0, p.i8)
    value = own[...] - jnp.log(predicted)
    for q in range(p.h):
        mean_out[q * p.i8 : (q + 1) * p.i8, :] = moved(value, -q * p.J)[:, 0 : p.J]
    clip = clip_of(p, sum_chunks(p, recv, p.S3, p.S3 - 1, 1))
    for t in range(p.R // LANES):
        values = []
        for b in range(p.hh):
            at = (t * p.hh + b) * p.S3 + p.i8
            values.append(recv[at : at + p.oi, :] + clip * recv[at + p.oi : at + 2 * p.oi, :])
        for o in range(p.hh):
            row = moved(values[0], -o * p.RL)
            for b in range(1, p.hh):
                row = jnp.where(block_mask(p.RL, p.oi, b), moved(values[b], (b - o) * p.RL), row)
            loyalty_out[o * p.oi : (o + 1) * p.oi, t * LANES : (t + 1) * LANES] = row


def local(
    mean_utility,
    market_share,
    product_traits,
    taste_draws,
    taste_scale,
    type_weight,
    market_size,
    product_firm,
    firm_order,
    loyalty,
    firm_share,
):
    p = Plan(
        lax.axis_size("mkt"),
        lax.axis_size("grp"),
        mean_utility.shape[0],
        mean_utility.shape[1],
        taste_scale.shape[0],
        firm_share.shape[1],
        firm_share.shape[0],
        loyalty.shape[0],
    )

    def exchange(x):
        return lax.all_to_all(x, "mkt", split_axis=0, concat_axis=0, tiled=True)

    def swap(x, bit):
        return lax.ppermute(x, "grp", [(q, q ^ bit) for q in range(p.Q)])

    order = firm_order.reshape(p.C, p.Q, p.own)
    order = jnp.pad(order, ((0, 0), (0, 0), (0, p.ownp - p.own)), constant_values=-1)
    order = order.reshape(p.C, p.Q, p.hh, p.oi).transpose(1, 2, 0, 3).reshape(p.Q * p.hh, p.C * p.oi)
    order = jnp.pad(order, ((0, 0), (0, LANES - p.C * p.oi)), constant_values=-1)
    if p.ownp > p.own:
        loyalty = jnp.pad(loyalty, ((0, p.ownp - p.own), (0, 0)))

    send = call(
        p,
        pack_kernel,
        sds((p.C * p.S, LANES)),
        (
            taste_scale,
            market_size,
            taste_draws.transpose(1, 0, 2),
            type_weight,
            loyalty,
            product_traits.transpose(2, 0, 1),
            product_firm,
            mean_utility,
            market_share,
        ),
        vmem=60,
        specs=[SM, SM] + [HBM] * 7,
        out_specs=HBM,
        scratch=(
            pltpu.VMEM((p.K, p.M, p.R), F32),
            pltpu.VMEM((p.M, p.R), F32),
            pltpu.VMEM((p.ownp, p.R), F32),
            pltpu.VMEM((p.K, p.M, p.J), F32),
            pltpu.VMEM((p.M, p.J), jnp.int32),
            pltpu.VMEM((p.M, p.J), F32),
            pltpu.VMEM((p.M, p.J), F32),
            pltpu.VMEM((p.C * p.S, LANES), F32),
            pltpu.SemaphoreType.DMA((7,)),
            pltpu.SemaphoreType.DMA((p.C,)),
        ),
    )
    tiles = sds((p.hh, p.J, LANES))
    firms_t, mean_t, shift_t, mass_t, mass_row, loy, draws_t, traits_t = call(
        p,
        prep_kernel,
        (
            tiles,
            tiles,
            tiles,
            sds((p.RL, p.ML)),
            sds((8, LANES)),
            sds((LANES, LANES)),
            sds((p.K, p.RL, p.ML)),
            sds((p.K, p.hh, p.J, LANES)),
        ),
        (exchange(send),),
        scratch=(pltpu.VMEM((max(LANES, p.PR), LANES), F32),),
    )
    rows = [loy]
    bit = 1
    while bit < p.Q:
        rows.append(swap(rows[0] if bit == 1 else jnp.concatenate(rows, axis=0), bit))
        bit *= 2
    taste, hot = call(
        p,
        taste_kernel,
        (sds((p.J, p.RL, p.ML)), sds((p.J, p.hh, p.F, LANES), BF)),
        (draws_t, traits_t, firms_t),
    )
    table, share, columns = call(
        p,
        table_kernel,
        (sds((p.FP, LANES)), sds((p.FP, LANES)), sds((p.hh, LANES, LANES))),
        (order, firm_share, *rows),
        specs=[VM, HBM] + [VM] * len(rows),
        scratch=(pltpu.VMEM((p.F, LANES), F32), pltpu.SemaphoreType.DMA(())),
    )
    half = sds((p.HR + 8, LANES))
    step_outs = (sds((p.PB, LANES)), half, half)
    step_scratch = step_scratch_of(p)
    fixed = (taste, hot, mass_t, mass_row)
    for step in range(ITERS):
        if step == 0:
            pred, keep, give = call(
                p,
                first_kernel,
                step_outs,
                (table, mean_t, *fixed),
                scratch=step_scratch,
            )
        else:
            table, mean_t, pred, keep, give = call(
                p,
                next_kernel,
                (sds((p.FP, LANES)), tiles) + step_outs,
                (recv, gap_mine, gap_other, table, mean_t, shift_t, *fixed),
                scratch=step_scratch,
            )
        mine = call(p, add_kernel, half, (keep, swap(give, 1)))
        bit = 2
        while 2 * bit < p.Q:
            mine = call(p, add_kernel, half, (mine, swap(mine, bit)))
            bit *= 2
        gap_mine = call(p, gap_kernel, half, (mine, swap(mine, bit), share))
        gap_other = swap(gap_mine, 1)
        if step < ITERS - 1:
            recv = exchange(call(p, send_kernel, sds((p.C * p.S2, LANES)), (gap_mine, gap_other, pred)))
    send, own = call(
        p,
        final_kernel,
        (sds((p.C * p.S3, LANES)), sds((p.i8, LANES))),
        (gap_mine, gap_other, table, columns, pred, mean_t, shift_t),
        scratch=(
            pltpu.VMEM((p.FP, LANES), F32),
            pltpu.VMEM((max(LANES, p.PR), LANES), F32),
            pltpu.VMEM((p.C, p.i8, LANES), F32),
        ),
    )
    mean_out, loyalty_out = call(
        p, out_kernel, (sds((p.M, p.J)), sds((p.ownp, p.R))), (exchange(send), own)
    )
    return (mean_out, loyalty_out[0 : p.own] if p.ownp > p.own else loyalty_out)


def solution(mesh):
    both = ("mkt", "grp")
    placed = (
        P(both, None),
        P(both, None),
        P(both, None, None),
        P(both, None, None),
        P(),
        P(both, None),
        P(both),
        P(both, None),
        P(),
        P(both, None),
        P(),
    )
    return jax.shard_map(
        local,
        mesh=mesh,
        in_specs=placed,
        out_specs=(P(both, None), P(both, None)),
        check_vma=False,
    )
```

```python
import functools

import jax
import jax.numpy as jnp
from jax import lax
from jax.experimental import pallas as pl
from jax.experimental.pallas import tpu as pltpu
from jax.sharding import PartitionSpec as P

ITERS = 3
LANES = 128
clip_target = 0.5
norm_eps = 1e-06
BF = jnp.bfloat16
F32 = jnp.float32


class Plan:
    def __init__(self, mkt, grp, own_markets, products, traits, types, firms, own_firms):
        self.C, self.Q = mkt, grp
        self.M, self.J, self.K = own_markets, products, traits
        self.R, self.F, self.own = types, firms, own_firms
        self.RL = types // mkt
        self.hh = LANES // self.RL
        self.ii = own_markets // self.hh
        self.h = LANES // products
        self.i8 = own_markets // self.h
        self.top = max(self.hh, self.h)
        self.w = own_markets // self.top
        self.ML = own_markets * mkt
        self.PR = mkt * self.i8
        self.FP = firms // self.hh
        self.HR = self.FP // 2
        self.ownp = -(-own_firms // self.hh) * self.hh
        self.oi = self.ownp // self.hh
        self.u = max(1, 256 // self.ML)
        self.NS = products // self.u
        self.per = min(16, self.NS)
        self.NR = max(LANES, 2 * self.RL)
        self.s_draws = 0
        self.s_mass = self.s_draws + traits * self.ii
        self.s_loy = self.s_mass + self.ii
        self.s_traits = self.s_loy + self.oi
        self.s_firms = self.s_traits + traits * self.i8
        self.s_mean = self.s_firms + self.i8
        self.s_shift = self.s_mean + self.i8
        self.S = -(-(self.s_shift + self.i8) // 8) * 8
        self.PB = self.hh * products
        self.PH = self.PB // 2
        self.S2 = self.PH + 8
        self.S3 = -(-(self.i8 + 2 * self.oi + 1) // 8) * 8
        self.vmem = 16 if firms * products * self.ML <= 2**22 else 58


VM = pl.BlockSpec(memory_space=pltpu.VMEM)
SM = pl.BlockSpec(memory_space=pltpu.SMEM)
HBM = pl.BlockSpec(memory_space=pltpu.HBM)


def call(p, kernel, outs, args, scratch=(), specs=None, out_specs=None, vmem=None):
    return pl.pallas_call(
        functools.partial(kernel, p),
        out_shape=outs,
        in_specs=specs or [VM] * len(args),
        out_specs=out_specs or jax.tree.map(lambda _: VM, outs),
        scratch_shapes=list(scratch),
        compiler_params=pltpu.CompilerParams(vmem_limit_bytes=(vmem or p.vmem) * 2**20),
    )(*args)


def sds(shape, dtype=F32):
    return jax.ShapeDtypeStruct(shape, dtype)


def block_mask(width, rows, b):
    return lax.broadcasted_iota(jnp.int32, (rows, LANES), 1) // width == b


def fold(p, x):
    total = x
    for b in range(1, p.hh):
        total = total + pltpu.roll(x, b * p.RL, 1)
    return total


def split2(x):
    a = x.astype(BF)
    return a, (x - a.astype(F32)).astype(BF)


def split3(x):
    a = x.astype(BF)
    b, c = split2(x - a.astype(F32))
    return a, b, c


def dot(a, b):
    return jnp.dot(a, b, preferred_element_type=F32)


def dot_t(a, b):
    return lax.dot_general(a, b, (((1,), (1,)), ((), ())), preferred_element_type=F32)


def moved(x, shift):
    return pltpu.roll(x, shift % LANES, 1) if shift % LANES else x


def pack_kernel(
    p, scale, size, draws_h, weight_h, loyalty_h, traits_h, firms_h, mean_h, share_h, out_h,
    draws, weight, loyalty, traits, firms, mean, share, out, sems, out_sems,
):
    pairs = (
        (draws_h, draws), (weight_h, weight), (traits_h, traits), (firms_h, firms),
        (mean_h, mean), (share_h, share), (loyalty_h, loyalty),
    )
    copies = [pltpu.make_async_copy(a, b, sems.at[n]) for n, (a, b) in enumerate(pairs)]
    for copy in copies:
        copy.start()
    for copy in copies:
        copy.wait()
    row = lax.broadcasted_iota(jnp.int32, (p.M, LANES), 0)
    column = jnp.zeros((p.M, LANES), F32)
    for m in range(p.M):
        column = jnp.where(row == m, size[m], column)
    mass_total = None
    tiles = []
    for t in range(p.R // LANES):
        tile = weight[:, t * LANES : (t + 1) * LANES] * column
        tiles.append(tile)
        mass_total = tile if mass_total is None else mass_total + tile
    mass_total = jnp.sum(mass_total, axis=1, keepdims=True)

    def by_type(tile_of, c, section, rows):
        tile, b = tile_of(c // p.hh), c % p.hh
        value = tile[0:rows, :] if not b else moved(tile, -b * p.RL)[0:rows, :]
        for q in range(1, p.hh):
            piece = moved(tile, (q - b) * p.RL)[q * rows : (q + 1) * rows, :]
            value = jnp.where(block_mask(p.RL, rows, q), piece, value)
        out[c * p.S + section : c * p.S + section + rows, :] = value

    def packed(x):
        return jnp.concatenate([x[q * p.i8 : (q + 1) * p.i8, :] for q in range(p.h)], axis=1)

    products = [packed(traits[k] * scale[k]) for k in range(p.K)]
    products += [packed(firms[...].astype(F32)), packed(mean[...])]
    products += [packed(jnp.log(share[...]) + jnp.log(mass_total))]
    sends = []
    for c in range(p.C):
        for k in range(p.K):
            by_type(lambda t: draws[k, :, t * LANES : (t + 1) * LANES], c, p.s_draws + k * p.ii, p.ii)
        by_type(lambda t: tiles[t], c, p.s_mass, p.ii)
        by_type(lambda t: loyalty[:, t * LANES : (t + 1) * LANES], c, p.s_loy, p.oi)
        for n, value in enumerate(products):
            at = c * p.S + p.s_traits + n * p.i8
            out[at : at + p.i8, :] = value
        part = pl.ds(c * p.S, p.S)
        copy = pltpu.make_async_copy(out.at[part], out_h.at[part], out_sems.at[c])
        copy.start()
        sends.append(copy)
    for copy in sends:
        copy.wait()


def prep_kernel(p, recv, firms_t, mean_t, shift_t, mass_t, mass_row, loy, draws_t, traits_t, nat):
    ta = p.top // p.hh

    def typed(section, store):
        for a in range(ta):
            for c in range(p.C):
                at = c * p.S + section + a * p.w
                nat[(a * p.C + c) * p.w : (a * p.C + c + 1) * p.w, :] = recv[at : at + p.w, :]
        flat = nat[0:LANES, :]
        turned = flat.T
        for b in range(p.hh):
            store(b, turned[b * p.RL : (b + 1) * p.RL, :])
        return flat

    def put_mass(b, value):
        mass_t[:, b * LANES : (b + 1) * LANES] = value

    flat = typed(p.s_mass, put_mass)
    row = jnp.sum(flat, axis=0, keepdims=True)
    mass_row[...] = fold(p, jnp.broadcast_to(row, (8, LANES)))
    for k in range(p.K):

        def put_draws(b, value):
            draws_t[k, :, b * LANES : (b + 1) * LANES] = value

        typed(p.s_draws + k * p.ii, put_draws)

    tb = p.top // p.h

    def product(section, store):
        for copy in range(max(1, LANES // p.PR)):
            for a in range(tb):
                for c in range(p.C):
                    at = c * p.S + section + a * p.w
                    to = copy * p.PR + (a * p.C + c) * p.w
                    nat[to : to + p.w, :] = recv[at : at + p.w, :]
        if p.PR >= LANES:
            per = p.PR // LANES
            for gi in range(per):
                turned = nat[gi * LANES : (gi + 1) * LANES, :].T
                for q in range(p.h):
                    store(q * per + gi, turned[q * p.J : (q + 1) * p.J, :])
        else:
            per = LANES // p.PR
            turned = nat[0:LANES, :].T
            for b in range(p.hh):
                value = turned[b * per * p.J : (b * per + 1) * p.J, :]
                for s in range(1, per):
                    at = (b * per + s) * p.J
                    value = jnp.where(block_mask(p.PR, p.J, s), turned[at : at + p.J, :], value)
                store(b, value)

    def into(ref):
        def store(b, value):
            ref[b] = value

        return store

    product(p.s_firms, into(firms_t))
    product(p.s_mean, into(mean_t))
    product(p.s_shift, into(shift_t))
    for k in range(p.K):
        product(p.s_traits + k * p.i8, into(traits_t.at[k]))
    loy[...] = jnp.zeros_like(loy)
    for c in range(p.C):
        loy[c * p.oi : (c + 1) * p.oi, :] = recv[c * p.S + p.s_loy : c * p.S + p.s_loy + p.oi, :]


def taste_kernel(p, draws_t, traits_t, firms_t, taste, hot):
    rows = min(p.F, 256)
    firm = lax.broadcasted_iota(jnp.int32, (rows, LANES), 0).astype(F32).astype(BF)

    def body(n, _):
        for v in range(p.u):
            j = n * p.u + v
            for b in range(p.hh):
                at = slice(b * LANES, (b + 1) * LANES)
                value = None
                for k in range(p.K):
                    term = traits_t[k, b, pl.ds(j, 1), :] * draws_t[k, :, at]
                    value = term if value is None else value + term
                taste[j, :, at] = value
                row = firms_t[b, pl.ds(j, 1), :]
                for base in range(0, p.F, rows):
                    want = jnp.broadcast_to(row - float(base), (rows, LANES)).astype(BF)
                    hot[j, b, base : base + rows, :] = jnp.where(firm == want, jnp.ones((), BF), jnp.zeros((), BF))
        return 0

    lax.fori_loop(0, p.NS, body, 0)


def table_kernel(p, order, share_h, *refs):
    blocks, (table, share, columns, tile, sem) = refs[:-5], refs[-5:]
    lane = lax.axis_index("mkt") * p.RL
    start = pl.multiple_of(lane // LANES * LANES, LANES)
    copy = pltpu.make_async_copy(share_h.at[:, pl.ds(start, LANES)], tile, sem)
    copy.start()
    firm = lax.broadcasted_iota(jnp.int32, (p.F, LANES), 0)
    total = jnp.zeros((p.F, LANES), F32)
    blocks = [ref[at : at + LANES, :] for ref in blocks for at in range(0, ref.shape[0], LANES)]
    for s, block in enumerate(blocks):
        pieces = jnp.concatenate(split3(block), axis=1)
        member = lax.axis_index("grp") ^ s
        for b in range(p.hh):
            hot = (firm == order[pl.ds(member * p.hh + b, 1), :]).astype(F32).astype(BF)
            found = dot(hot, pieces)
            found = found[:, 0:LANES] + found[:, LANES : 2 * LANES] + found[:, 2 * LANES :]
            if p.hh > 1:
                found = jnp.where(block_mask(p.RL, p.F, b), found, 0.0)
            total = total + found
    pack_table(p, fold(p, total), table)
    for b in range(p.hh):
        row = order[pl.ds(lax.axis_index("grp") * p.hh + b, 1), :].astype(F32)
        columns[b] = jnp.broadcast_to(row, (LANES, LANES)).T
    copy.wait()
    if p.hh == 1:
        share[...] = tile[...]
    else:
        for b in range(p.hh):
            part = pltpu.roll(tile[b * p.FP : (b + 1) * p.FP, :], (b * p.RL + LANES - (lane - start)) % LANES, 1)
            mask = block_mask(p.RL, p.FP, b)
            share[...] = part if not b else jnp.where(mask, part, share[...])


def pack_table(p, full, out):
    value = full[0 : p.FP, :]
    for b in range(1, p.hh):
        value = jnp.where(block_mask(p.RL, p.FP, b), full[b * p.FP : (b + 1) * p.FP, :], value)
    out[...] = value


def clip_of(p, squares):
    return jnp.minimum(1.0, clip_target / jnp.sqrt(squares / (p.F * p.R) + norm_eps))


def sum_chunks(p, recv, step, start, rows):
    total = recv[start : start + rows, :]
    for c in range(1, p.C):
        total = total + recv[c * step + start : c * step + start + rows, :]
    return total


def step_body(p, table, mean_of, taste, hot, mass_t, mass_row, pred, parts, give, tab, expu, acc):
    turned = table[...].T
    for q, piece in enumerate(split2(turned)):
        for t in range(p.F // LANES):
            b, at = divmod(t * LANES, p.FP)
            tab[t, q * p.RL : (q + 1) * p.RL, :] = piece[b * p.RL : (b + 1) * p.RL, at : at + LANES]

    def hot_of(n):
        return jnp.concatenate([hot[n * p.u + v, b] for v in range(p.u) for b in range(p.hh)], axis=1)

    def gather(n, total):
        found = dot(jnp.concatenate([tab[t] for t in range(p.F // LANES)], axis=1), hot_of(n))
        found = found[0 : p.RL] + found[p.RL : 2 * p.RL]
        for v in range(p.u):
            j = n * p.u + v
            means = [jnp.broadcast_to(mean_of[b, pl.ds(j, 1), :], (p.RL, LANES)) for b in range(p.hh)]
            means = means[0] if p.hh == 1 else jnp.concatenate(means, axis=1)
            e = jnp.exp(taste[j] + found[:, v * p.ML : (v + 1) * p.ML] + means)
            expu[j] = e
            total = total + e
        return total

    total = lax.fori_loop(0, p.NS, gather, jnp.zeros((p.RL, p.ML), F32), unroll=min(16, p.NS))
    scale = mass_t[...] / (1.0 + total)
    if p.NR > 2 * p.RL:
        parts[...] = jnp.zeros_like(parts)

    def fill(n):
        for v in range(p.u):
            j = n * p.u + v
            x = expu[j] * scale
            hi, lo = split2(x)
            for b in range(p.hh):
                at = slice(b * LANES, (b + 1) * LANES)
                parts[n, v * p.hh + b, 0 : p.RL, :] = hi[:, at]
                parts[n, v * p.hh + b, p.RL : 2 * p.RL, :] = lo[:, at]
            row = jnp.sum(x, axis=0, keepdims=True)
            for b in range(p.hh):
                pred[pl.ds(b * p.J + j, 1), :] = row[:, b * LANES : (b + 1) * LANES]

    give[0 : p.HR, :] = totals_of(p, parts, hot, acc, 1, fill)
    give[p.HR :, :] = mass_row[...]


def totals_of(p, parts, hot, acc, other, fill):
    start = ((lax.axis_index("grp") & 1) ^ other) * p.HR
    acc[...] = jnp.zeros_like(acc)

    def body(n, _):
        value = None
        for s in range(p.per):
            at = n * p.per + s
            fill(at)
            left = []
            for v in range(p.u):
                for b in range(p.hh):
                    rows = [pl.ds(pl.multiple_of(start + fh * p.FP, 8), p.HR) for fh in range(p.hh)]
                    tall = [hot[at * p.u + v, b, r, :] for r in rows]
                    left.append(tall[0] if p.hh == 1 else jnp.concatenate(tall, axis=0))
            right = jnp.concatenate([parts[at, t] for t in range(p.u * p.hh)], axis=1)
            term = dot_t(jnp.concatenate(left, axis=1), right)
            value = term if value is None else value + term
        acc[...] += value
        return 0

    lax.fori_loop(0, p.NS // p.per, body, 0)
    full = acc[:, 0:LANES]
    for t in range(1, p.NR // LANES):
        full = full + acc[:, t * LANES : (t + 1) * LANES]
    full = fold(p, full)
    value = full[0 : p.HR, :]
    for b in range(1, p.hh):
        value = jnp.where(block_mask(p.RL, p.HR, b), full[b * p.HR : (b + 1) * p.HR, :], value)
    return value


def rest_kernel(p, parts, hot, mass_row, keep, acc):
    keep[0 : p.HR, :] = totals_of(p, parts, hot, acc, 0, lambda n: None)
    keep[p.HR :, :] = mass_row[...]


def step_scratch_of(p):
    return (
        pltpu.VMEM((p.F // LANES, 2 * p.RL, LANES), BF),
        pltpu.VMEM((p.J, p.RL, p.ML), F32),
        pltpu.VMEM((p.F // 2, p.NR), F32),
    )


def split_predicted(p, pred, pred_keep, pred_give):
    mine = (lax.axis_index("mkt") & 1) * p.PH
    pred_keep[...] = pred[pl.ds(pl.multiple_of(mine, 8), p.PH), :]
    pred_give[...] = pred[pl.ds(pl.multiple_of(p.PH - mine, 8), p.PH), :]


def first_kernel(
    p, table, mean_t, taste, hot, mass_t, mass_row, pred_keep, pred_give, parts, give, pred, *scratch
):
    step_body(p, table, mean_t, taste, hot, mass_t, mass_row, pred, parts, give, *scratch)
    split_predicted(p, pred, pred_keep, pred_give)


def update(p, recv, gap_mine, gap_other, table_in, mean_in, shift_t, table, mean_t):
    clip = clip_of(p, sum_chunks(p, recv, p.S2, p.PH, 1))
    mine = (lax.axis_index("grp") & 1) * p.HR
    for ref, start in ((gap_mine, mine), (gap_other, p.HR - mine)):
        at = pl.ds(pl.multiple_of(start, 8), p.HR)
        table[at, :] = table_in[at, :] + clip * ref[0 : p.HR, :]
    halves = []
    for side in range(2):
        total = recv[side * p.S2 : side * p.S2 + p.PH, :]
        for c in range(side + 2, p.C, 2):
            total = total + recv[c * p.S2 : c * p.S2 + p.PH, :]
        halves.append(total)
    total = jnp.log(jnp.concatenate(halves, axis=0))
    for b in range(p.hh):
        mean_t[b] = mean_in[b] + shift_t[b] - total[b * p.J : (b + 1) * p.J, :]


def next_kernel(
    p, recv, gap_mine, gap_other, table_in, mean_in, shift_t, taste, hot, mass_t, mass_row,
    table, mean_t, pred_keep, pred_give, parts, give, pred, *scratch
):
    update(p, recv, gap_mine, gap_other, table_in, mean_in, shift_t, table, mean_t)
    step_body(p, table, mean_t, taste, hot, mass_t, mass_row, pred, parts, give, *scratch)
    split_predicted(p, pred, pred_keep, pred_give)


def last_kernel(
    p, recv, gap_mine, gap_other, table_in, mean_in, shift_t, taste, hot, mass_t, mass_row,
    table, mean_t, pred, parts, give, *scratch
):
    update(p, recv, gap_mine, gap_other, table_in, mean_in, shift_t, table, mean_t)
    step_body(p, table, mean_t, taste, hot, mass_t, mass_row, pred, parts, give, *scratch)


def add_kernel(p, a, b, *refs):
    refs[len(refs) // 2][...] = a[...] + b[...]
    for n in range(len(refs) // 2):
        refs[len(refs) // 2 + 1 + n][...] = refs[n][...]


def gap_kernel(p, mine, other, share, *refs):
    gap = refs[-1] if len(refs) == 1 else refs[2]
    if len(refs) > 1:
        refs[3][...] = refs[0][...] + refs[1][...]
    total = mine[...] + other[...]
    at = pl.ds(pl.multiple_of((lax.axis_index("grp") & 1) * p.HR, 8), p.HR)
    value = jnp.log(share[at, :]) - jnp.log(total[0 : p.HR, :] / total[p.HR : p.HR + 1, :])
    gap[0 : p.HR, :] = value
    rows = jnp.sum(value * value, axis=0, keepdims=True)
    gap[p.HR :, :] = jnp.broadcast_to(jnp.sum(rows, axis=1, keepdims=True), (8, LANES))


def send_kernel(p, gap_mine, gap_other, pred, send):
    squares = gap_mine[p.HR :, :] + gap_other[p.HR :, :]
    value = pred[...]
    for c in range(p.C):
        send[c * p.S2 : c * p.S2 + p.PH, :] = value
        send[c * p.S2 + p.PH : (c + 1) * p.S2, :] = squares


def final_kernel(p, gap_mine, gap_other, table, columns, pred, mean_t, shift_t, send, own, gap, nat, means):
    mine = (lax.axis_index("grp") & 1) * p.HR
    for ref, start in ((gap_mine, mine), (gap_other, p.HR - mine)):
        gap[pl.ds(pl.multiple_of(start, 8), p.HR), :] = ref[0 : p.HR, :]
    squares = gap_mine[p.HR : p.HR + 1, :] + gap_other[p.HR : p.HR + 1, :]
    lane = lax.broadcasted_iota(jnp.int32, (LANES, LANES), 1).astype(F32)
    for n, ref in enumerate((table, gap)):
        pieces = jnp.concatenate(split3(ref[...]), axis=1)
        picked = None
        for o in range(p.hh):
            total = None
            for b in range(p.hh):
                wide = -(-p.FP // LANES)
                hot = [columns[o] == lane + float(b * p.FP + t * LANES) for t in range(wide)]
                hot = jnp.concatenate([x.astype(F32).astype(BF) for x in hot], axis=1)[:, 0 : p.FP]
                found = dot(hot, pieces)
                found = found[:, 0:LANES] + found[:, LANES : 2 * LANES] + found[:, 2 * LANES :]
                if p.hh > 1:
                    found = jnp.where(block_mask(p.RL, LANES, b), found, 0.0)
                total = found if total is None else total + found
            total = fold(p, total)
            picked = total if picked is None else jnp.where(block_mask(p.RL, LANES, o), total, picked)
        at = p.i8 + n * p.oi
        for c in range(p.C):
            send[c * p.S3 + at : c * p.S3 + at + p.oi, :] = picked[c * p.oi : (c + 1) * p.oi, :]
    tb = p.top // p.h

    def by_owner(block, store):
        if p.PR >= LANES:
            per = p.PR // LANES
            for gi in range(per):
                tall = [block(q * per + gi) for q in range(p.h)]
                nat[gi * LANES : (gi + 1) * LANES, :] = jnp.concatenate(tall, axis=0).T
        else:
            per = LANES // p.PR
            tall = [moved(block(q // per), -(q % per) * p.PR) for q in range(p.h)]
            nat[0:LANES, :] = jnp.concatenate(tall, axis=0).T
        for c in range(p.C):
            for a in range(tb):
                at = (a * p.C + c) * p.w
                store(c, slice(a * p.w, (a + 1) * p.w), nat[at : at + p.w, :])

    def put_mean(c, at, value):
        means[c, at, :] = value

    def put_pred(c, at, value):
        send[c * p.S3 + at.start : c * p.S3 + at.stop, :] = value

    by_owner(lambda b: mean_t[b] + shift_t[b], put_mean)
    by_owner(lambda b: pred[b * p.J : (b + 1) * p.J, :], put_pred)
    own[...] = means[lax.axis_index("mkt")]
    for c in range(p.C):
        send[(c + 1) * p.S3 - 1 : (c + 1) * p.S3, :] = squares


def out_kernel(p, recv, own, mean_out, loyalty_out):
    predicted = sum_chunks(p, recv, p.S3, 0, p.i8)
    value = own[...] - jnp.log(predicted)
    for q in range(p.h):
        mean_out[q * p.i8 : (q + 1) * p.i8, :] = moved(value, -q * p.J)[:, 0 : p.J]
    clip = clip_of(p, sum_chunks(p, recv, p.S3, p.S3 - 1, 1))
    for t in range(p.R // LANES):
        values = []
        for b in range(p.hh):
            at = (t * p.hh + b) * p.S3 + p.i8
            values.append(recv[at : at + p.oi, :] + clip * recv[at + p.oi : at + 2 * p.oi, :])
        for o in range(p.hh):
            row = moved(values[0], -o * p.RL)
            for b in range(1, p.hh):
                row = jnp.where(block_mask(p.RL, p.oi, b), moved(values[b], (b - o) * p.RL), row)
            loyalty_out[o * p.oi : (o + 1) * p.oi, t * LANES : (t + 1) * LANES] = row


def local(
    mean_utility,
    market_share,
    product_traits,
    taste_draws,
    taste_scale,
    type_weight,
    market_size,
    product_firm,
    firm_order,
    loyalty,
    firm_share,
):
    p = Plan(
        lax.axis_size("mkt"),
        lax.axis_size("grp"),
        mean_utility.shape[0],
        mean_utility.shape[1],
        taste_scale.shape[0],
        firm_share.shape[1],
        firm_share.shape[0],
        loyalty.shape[0],
    )

    def exchange(x):
        return lax.all_to_all(x, "mkt", split_axis=0, concat_axis=0, tiled=True)

    def swap(x, bit):
        return lax.ppermute(x, "grp", [(q, q ^ bit) for q in range(p.Q)])

    order = firm_order.reshape(p.C, p.Q, p.own)
    order = jnp.pad(order, ((0, 0), (0, 0), (0, p.ownp - p.own)), constant_values=-1)
    order = order.reshape(p.C, p.Q, p.hh, p.oi).transpose(1, 2, 0, 3).reshape(p.Q * p.hh, p.C * p.oi)
    order = jnp.pad(order, ((0, 0), (0, LANES - p.C * p.oi)), constant_values=-1)
    if p.ownp > p.own:
        loyalty = jnp.pad(loyalty, ((0, p.ownp - p.own), (0, 0)))

    send = call(
        p,
        pack_kernel,
        sds((p.C * p.S, LANES)),
        (
            taste_scale,
            market_size,
            taste_draws.transpose(1, 0, 2),
            type_weight,
            loyalty,
            product_traits.transpose(2, 0, 1),
            product_firm,
            mean_utility,
            market_share,
        ),
        vmem=60,
        specs=[SM, SM] + [HBM] * 7,
        out_specs=HBM,
        scratch=(
            pltpu.VMEM((p.K, p.M, p.R), F32),
            pltpu.VMEM((p.M, p.R), F32),
            pltpu.VMEM((p.ownp, p.R), F32),
            pltpu.VMEM((p.K, p.M, p.J), F32),
            pltpu.VMEM((p.M, p.J), jnp.int32),
            pltpu.VMEM((p.M, p.J), F32),
            pltpu.VMEM((p.M, p.J), F32),
            pltpu.VMEM((p.C * p.S, LANES), F32),
            pltpu.SemaphoreType.DMA((7,)),
            pltpu.SemaphoreType.DMA((p.C,)),
        ),
    )
    tiles = sds((p.hh, p.J, LANES))
    firms_t, mean_t, shift_t, mass_t, mass_row, loy, draws_t, traits_t = call(
        p,
        prep_kernel,
        (
            tiles,
            tiles,
            tiles,
            sds((p.RL, p.ML)),
            sds((8, LANES)),
            sds((LANES, LANES)),
            sds((p.K, p.RL, p.ML)),
            sds((p.K, p.hh, p.J, LANES)),
        ),
        (exchange(send),),
        scratch=(pltpu.VMEM((max(LANES, p.PR), LANES), F32),),
    )
    rows = [loy] + [swap(loy, bits) for bits in range(1, p.Q)]
    taste, hot = call(
        p,
        taste_kernel,
        (sds((p.J, p.RL, p.ML)), sds((p.J, p.hh, p.F, LANES), BF)),
        (draws_t, traits_t, firms_t),
    )
    table, share, columns = call(
        p,
        table_kernel,
        (sds((p.FP, LANES)), sds((p.FP, LANES)), sds((p.hh, LANES, LANES))),
        (order, firm_share, *rows),
        specs=[VM, HBM] + [VM] * len(rows),
        scratch=(pltpu.VMEM((p.F, LANES), F32), pltpu.SemaphoreType.DMA(())),
    )
    half = sds((p.HR + 8, LANES))
    tables = (sds((p.FP, LANES)), tiles)
    half_pred = sds((p.PH, LANES))
    all_parts = sds((p.NS, p.u * p.hh, p.NR, LANES), BF)
    step_scratch = step_scratch_of(p)
    whole_pred = (pltpu.VMEM((p.PB, LANES), F32),)
    fixed = (taste, hot, mass_t, mass_row)
    for step in range(ITERS):
        last = step == ITERS - 1
        if step == 0:
            pred, pred_give, parts, give = call(
                p,
                first_kernel,
                (half_pred, half_pred, all_parts, half),
                (table, mean_t, *fixed),
                scratch=whole_pred + step_scratch,
            )
        elif not last:
            table, mean_t, pred, pred_give, parts, give = call(
                p,
                next_kernel,
                tables + (half_pred, half_pred, all_parts, half),
                (recv, gap_mine, gap_other, table, mean_t, shift_t, *fixed),
                scratch=whole_pred + step_scratch,
            )
        else:
            table, mean_t, pred, parts, give = call(
                p,
                last_kernel,
                tables + (sds((p.PB, LANES)), all_parts, half),
                (recv, gap_mine, gap_other, table, mean_t, shift_t, *fixed),
                scratch=step_scratch,
            )
        given = swap(give, 1)
        keep = call(p, rest_kernel, half, (parts, hot, mass_row), scratch=step_scratch[-1:])
        if last:
            (mine,) = call(p, add_kernel, (half,), (keep, given))
        else:
            mine, pred_give = call(p, add_kernel, (half, half_pred), (keep, given, pred_give))
            pred_other = lax.ppermute(pred_give, "mkt", [(c, c ^ 1) for c in range(p.C)])
        bit = 2
        while 2 * bit < p.Q:
            (mine,) = call(p, add_kernel, (half,), (mine, swap(mine, bit)))
            bit *= 2
        sums = (mine, swap(mine, bit), share)
        if last:
            gap_mine = call(p, gap_kernel, half, sums)
        else:
            gap_mine, pred = call(p, gap_kernel, (half, half_pred), sums + (pred, pred_other))
        gap_other = swap(gap_mine, 1)
        if not last:
            recv = exchange(
                call(p, send_kernel, sds((p.C * p.S2, LANES)), (gap_mine, gap_other, pred))
            )
    send, own = call(
        p,
        final_kernel,
        (sds((p.C * p.S3, LANES)), sds((p.i8, LANES))),
        (gap_mine, gap_other, table, columns, pred, mean_t, shift_t),
        scratch=(
            pltpu.VMEM((p.FP, LANES), F32),
            pltpu.VMEM((max(LANES, p.PR), LANES), F32),
            pltpu.VMEM((p.C, p.i8, LANES), F32),
        ),
    )
    mean_out, loyalty_out = call(
        p, out_kernel, (sds((p.M, p.J)), sds((p.ownp, p.R))), (exchange(send), own)
    )
    return (mean_out, loyalty_out[0 : p.own] if p.ownp > p.own else loyalty_out)


def solution(mesh):
    both = ("mkt", "grp")
    placed = (
        P(both, None),
        P(both, None),
        P(both, None, None),
        P(both, None, None),
        P(),
        P(both, None),
        P(both),
        P(both, None),
        P(),
        P(both, None),
        P(),
    )
    return jax.shard_map(
        local,
        mesh=mesh,
        in_specs=placed,
        out_specs=(P(both, None), P(both, None)),
        check_vma=False,
    )
```

```python
import functools

import jax
import jax.numpy as jnp
from jax import lax
from jax.experimental import pallas as pl
from jax.experimental.pallas import tpu as pltpu
from jax.sharding import PartitionSpec as P

ITERS = 3
LANES = 128
clip_target = 0.5
norm_eps = 1e-06
BF = jnp.bfloat16
F32 = jnp.float32


class Plan:
    def __init__(self, mkt, grp, own_markets, products, traits, types, firms, own_firms):
        self.C, self.Q = mkt, grp
        self.M, self.J, self.K = own_markets, products, traits
        self.R, self.F, self.own = types, firms, own_firms
        self.RL = types // mkt
        self.hh = LANES // self.RL
        self.ii = own_markets // self.hh
        self.h = LANES // products
        self.i8 = own_markets // self.h
        self.top = max(self.hh, self.h)
        self.w = own_markets // self.top
        self.ML = own_markets * mkt
        self.PR = mkt * self.i8
        self.FP = firms // self.hh
        self.HR = self.FP // 2
        self.ownp = -(-own_firms // self.hh) * self.hh
        self.oi = self.ownp // self.hh
        self.u = max(1, 256 // self.ML)
        self.NS = products // self.u
        self.per = self.NS if self.NS <= 32 else 16
        self.NR = max(LANES, 2 * self.RL)
        self.s_draws = 0
        self.s_mass = self.s_draws + traits * self.ii
        self.s_loy = self.s_mass + self.ii
        self.s_traits = self.s_loy + self.oi
        self.s_firms = self.s_traits + traits * self.i8
        self.s_mean = self.s_firms + self.i8
        self.s_shift = self.s_mean + self.i8
        self.S = -(-(self.s_shift + self.i8) // 8) * 8
        self.PB = self.hh * products
        self.PH = self.PB // 2
        self.S2 = self.PH + 8
        self.S3 = -(-(self.i8 + 2 * self.oi + 1) // 8) * 8
        self.vmem = 16 if firms * products * self.ML <= 2**22 else 58


VM = pl.BlockSpec(memory_space=pltpu.VMEM)
HBM = pl.BlockSpec(memory_space=pltpu.HBM)


def call(p, kernel, outs, args, scratch=(), specs=None, out_specs=None, vmem=None):
    return pl.pallas_call(
        functools.partial(kernel, p),
        out_shape=outs,
        in_specs=specs or [VM] * len(args),
        out_specs=out_specs or jax.tree.map(lambda _: VM, outs),
        scratch_shapes=list(scratch),
        compiler_params=pltpu.CompilerParams(vmem_limit_bytes=(vmem or p.vmem) * 2**20),
    )(*args)


def sds(shape, dtype=F32):
    return jax.ShapeDtypeStruct(shape, dtype)


def block_mask(width, rows, b):
    return lax.broadcasted_iota(jnp.int32, (rows, LANES), 1) // width == b


def fold(p, x):
    total = x
    for b in range(1, p.hh):
        total = total + pltpu.roll(x, b * p.RL, 1)
    return total


def split2(x):
    a = x.astype(BF)
    return a, (x - a.astype(F32)).astype(BF)


def split3(x):
    a = x.astype(BF)
    b, c = split2(x - a.astype(F32))
    return a, b, c


def dot(a, b):
    return jnp.dot(a, b, preferred_element_type=F32)


def dot_t(a, b):
    return lax.dot_general(a, b, (((1,), (1,)), ((), ())), preferred_element_type=F32)


def moved(x, shift):
    return pltpu.roll(x, shift % LANES, 1) if shift % LANES else x


def pack_kernel(
    p, scale_h, size_h, draws_h, weight_h, loyalty_h, traits_h, firms_h, mean_h, share_h, out_h,
    draws, weight, loyalty, traits, firms, mean, share, out, scale, size, sems, out_sems,
):
    pairs = (
        (draws_h, draws), (weight_h, weight), (traits_h, traits), (firms_h, firms),
        (mean_h, mean), (share_h, share), (loyalty_h, loyalty), (scale_h, scale), (size_h, size),
    )
    copies = [pltpu.make_async_copy(a, b, sems.at[n]) for n, (a, b) in enumerate(pairs)]
    for copy in copies:
        copy.start()
    for copy in copies:
        copy.wait()
    row = lax.broadcasted_iota(jnp.int32, (p.M, LANES), 0)
    column = jnp.zeros((p.M, LANES), F32)
    for m in range(p.M):
        column = jnp.where(row == m, size[m], column)
    mass_total = None
    tiles = []
    for t in range(p.R // LANES):
        tile = weight[:, t * LANES : (t + 1) * LANES] * column
        tiles.append(tile)
        mass_total = tile if mass_total is None else mass_total + tile
    mass_total = jnp.sum(mass_total, axis=1, keepdims=True)

    def by_type(tile_of, c, section, rows):
        tile, b = tile_of(c // p.hh), c % p.hh
        value = tile[0:rows, :] if not b else moved(tile, -b * p.RL)[0:rows, :]
        for q in range(1, p.hh):
            piece = moved(tile, (q - b) * p.RL)[q * rows : (q + 1) * rows, :]
            value = jnp.where(block_mask(p.RL, rows, q), piece, value)
        out[c * p.S + section : c * p.S + section + rows, :] = value

    def packed(x):
        return jnp.concatenate([x[q * p.i8 : (q + 1) * p.i8, :] for q in range(p.h)], axis=1)

    products = [packed(traits[k] * scale[k]) for k in range(p.K)]
    products += [packed(firms[...].astype(F32)), packed(mean[...])]
    products += [packed(jnp.log(share[...]) + jnp.log(mass_total))]
    sends = []
    for c in range(p.C):
        for k in range(p.K):
            by_type(lambda t: draws[k, :, t * LANES : (t + 1) * LANES], c, p.s_draws + k * p.ii, p.ii)
        by_type(lambda t: tiles[t], c, p.s_mass, p.ii)
        by_type(lambda t: loyalty[:, t * LANES : (t + 1) * LANES], c, p.s_loy, p.oi)
        for n, value in enumerate(products):
            at = c * p.S + p.s_traits + n * p.i8
            out[at : at + p.i8, :] = value
        part = pl.ds(c * p.S, p.S)
        copy = pltpu.make_async_copy(out.at[part], out_h.at[part], out_sems.at[c])
        copy.start()
        sends.append(copy)
    for copy in sends:
        copy.wait()


def prep_kernel(p, recv, firms_t, mean_t, shift_t, mass_t, mass_row, loy, draws_t, traits_t, nat):
    ta = p.top // p.hh

    def typed(section, store):
        for a in range(ta):
            for c in range(p.C):
                at = c * p.S + section + a * p.w
                nat[(a * p.C + c) * p.w : (a * p.C + c + 1) * p.w, :] = recv[at : at + p.w, :]
        flat = nat[0:LANES, :]
        turned = flat.T
        for b in range(p.hh):
            store(b, turned[b * p.RL : (b + 1) * p.RL, :])
        return flat

    def put_mass(b, value):
        mass_t[:, b * LANES : (b + 1) * LANES] = value

    flat = typed(p.s_mass, put_mass)
    row = jnp.sum(flat, axis=0, keepdims=True)
    mass_row[...] = fold(p, jnp.broadcast_to(row, (8, LANES)))
    for k in range(p.K):

        def put_draws(b, value):
            draws_t[k, :, b * LANES : (b + 1) * LANES] = value

        typed(p.s_draws + k * p.ii, put_draws)

    tb = p.top // p.h

    def product(section, store):
        for copy in range(max(1, LANES // p.PR)):
            for a in range(tb):
                for c in range(p.C):
                    at = c * p.S + section + a * p.w
                    to = copy * p.PR + (a * p.C + c) * p.w
                    nat[to : to + p.w, :] = recv[at : at + p.w, :]
        if p.PR >= LANES:
            per = p.PR // LANES
            for gi in range(per):
                turned = nat[gi * LANES : (gi + 1) * LANES, :].T
                for q in range(p.h):
                    store(q * per + gi, turned[q * p.J : (q + 1) * p.J, :])
        else:
            per = LANES // p.PR
            turned = nat[0:LANES, :].T
            for b in range(p.hh):
                value = turned[b * per * p.J : (b * per + 1) * p.J, :]
                for s in range(1, per):
                    at = (b * per + s) * p.J
                    value = jnp.where(block_mask(p.PR, p.J, s), turned[at : at + p.J, :], value)
                store(b, value)

    def into(ref):
        def store(b, value):
            ref[b] = value

        return store

    product(p.s_firms, into(firms_t))
    product(p.s_mean, into(mean_t))
    product(p.s_shift, into(shift_t))
    for k in range(p.K):
        product(p.s_traits + k * p.i8, into(traits_t.at[k]))
    loy[...] = jnp.zeros_like(loy)
    for c in range(p.C):
        loy[c * p.oi : (c + 1) * p.oi, :] = recv[c * p.S + p.s_loy : c * p.S + p.s_loy + p.oi, :]


def taste_kernel(p, draws_t, traits_t, firms_t, taste, hot):
    rows = min(p.F, 256)
    firm = lax.broadcasted_iota(jnp.int32, (rows, LANES), 0).astype(F32).astype(BF)

    def body(n, _):
        for v in range(p.u):
            j = n * p.u + v
            for b in range(p.hh):
                at = slice(b * LANES, (b + 1) * LANES)
                value = None
                for k in range(p.K):
                    term = traits_t[k, b, pl.ds(j, 1), :] * draws_t[k, :, at]
                    value = term if value is None else value + term
                taste[j, :, at] = value
                row = firms_t[b, pl.ds(j, 1), :]
                for base in range(0, p.F, rows):
                    want = jnp.broadcast_to(row - float(base), (rows, LANES)).astype(BF)
                    hot[j, b, base : base + rows, :] = jnp.where(firm == want, jnp.ones((), BF), jnp.zeros((), BF))
        return 0

    lax.fori_loop(0, p.NS, body, 0)


def table_kernel(p, order, share_h, *refs):
    blocks, (table, share, columns, tile, sem) = refs[:-5], refs[-5:]
    lane = lax.axis_index("mkt") * p.RL
    start = pl.multiple_of(lane // LANES * LANES, LANES)
    copy = pltpu.make_async_copy(share_h.at[:, pl.ds(start, LANES)], tile, sem)
    copy.start()
    firm = lax.broadcasted_iota(jnp.int32, (p.F, LANES), 0)
    total = jnp.zeros((p.F, LANES), F32)
    blocks = [ref[at : at + LANES, :] for ref in blocks for at in range(0, ref.shape[0], LANES)]
    for s, block in enumerate(blocks):
        pieces = jnp.concatenate(split3(block), axis=1)
        member = lax.axis_index("grp") ^ s
        for b in range(p.hh):
            hot = (firm == order[pl.ds(member * p.hh + b, 1), :]).astype(F32).astype(BF)
            found = dot(hot, pieces)
            found = found[:, 0:LANES] + found[:, LANES : 2 * LANES] + found[:, 2 * LANES :]
            if p.hh > 1:
                found = jnp.where(block_mask(p.RL, p.F, b), found, 0.0)
            total = total + found
    pack_table(p, fold(p, total), table)
    for b in range(p.hh):
        row = order[pl.ds(lax.axis_index("grp") * p.hh + b, 1), :].astype(F32)
        columns[b] = jnp.broadcast_to(row, (LANES, LANES)).T
    copy.wait()
    if p.hh == 1:
        share[...] = tile[...]
    else:
        for b in range(p.hh):
            part = pltpu.roll(tile[b * p.FP : (b + 1) * p.FP, :], (b * p.RL + LANES - (lane - start)) % LANES, 1)
            mask = block_mask(p.RL, p.FP, b)
            share[...] = part if not b else jnp.where(mask, part, share[...])


def pack_table(p, full, out):
    value = full[0 : p.FP, :]
    for b in range(1, p.hh):
        value = jnp.where(block_mask(p.RL, p.FP, b), full[b * p.FP : (b + 1) * p.FP, :], value)
    out[...] = value


def clip_of(p, squares):
    return jnp.minimum(1.0, clip_target / jnp.sqrt(squares / (p.F * p.R) + norm_eps))


def sum_chunks(p, recv, step, start, rows):
    total = recv[start : start + rows, :]
    for c in range(1, p.C):
        total = total + recv[c * step + start : c * step + start + rows, :]
    return total


def step_body(p, table, mean_of, taste, hot, mass_t, mass_row, pred, parts, give, tab, expu, acc):
    turned = table[...].T
    for q, piece in enumerate(split2(turned)):
        for t in range(p.F // LANES):
            b, at = divmod(t * LANES, p.FP)
            tab[t, q * p.RL : (q + 1) * p.RL, :] = piece[b * p.RL : (b + 1) * p.RL, at : at + LANES]

    def hot_of(n):
        return jnp.concatenate([hot[n * p.u + v, b] for v in range(p.u) for b in range(p.hh)], axis=1)

    def gather(n, total):
        found = dot(jnp.concatenate([tab[t] for t in range(p.F // LANES)], axis=1), hot_of(n))
        found = found[0 : p.RL] + found[p.RL : 2 * p.RL]
        for v in range(p.u):
            j = n * p.u + v
            means = [jnp.broadcast_to(mean_of[b, pl.ds(j, 1), :], (p.RL, LANES)) for b in range(p.hh)]
            means = means[0] if p.hh == 1 else jnp.concatenate(means, axis=1)
            e = jnp.exp(taste[j] + found[:, v * p.ML : (v + 1) * p.ML] + means)
            expu[j] = e
            total = total + e
        return total

    total = lax.fori_loop(0, p.NS, gather, jnp.zeros((p.RL, p.ML), F32), unroll=min(16, p.NS))
    scale = mass_t[...] / (1.0 + total)
    if p.NR > 2 * p.RL:
        parts[...] = jnp.zeros_like(parts)

    def fill(n):
        for v in range(p.u):
            j = n * p.u + v
            x = expu[j] * scale
            hi, lo = split2(x)
            for b in range(p.hh):
                at = slice(b * LANES, (b + 1) * LANES)
                parts[n, v * p.hh + b, 0 : p.RL, :] = hi[:, at]
                parts[n, v * p.hh + b, p.RL : 2 * p.RL, :] = lo[:, at]
            row = jnp.sum(x, axis=0, keepdims=True)
            for b in range(p.hh):
                pred[pl.ds(b * p.J + j, 1), :] = row[:, b * LANES : (b + 1) * LANES]

    give[0 : p.HR, :] = totals_of(p, parts, hot, acc, 1, fill)
    give[p.HR :, :] = mass_row[...]


def totals_of(p, parts, hot, acc, other, fill):
    start = ((lax.axis_index("grp") & 1) ^ other) * p.HR
    acc[...] = jnp.zeros_like(acc)

    def body(n, _):
        value = None
        for s in range(p.per):
            at = n * p.per + s
            fill(at)
            left = []
            for v in range(p.u):
                for b in range(p.hh):
                    rows = [pl.ds(pl.multiple_of(start + fh * p.FP, 8), p.HR) for fh in range(p.hh)]
                    tall = [hot[at * p.u + v, b, r, :] for r in rows]
                    left.append(tall[0] if p.hh == 1 else jnp.concatenate(tall, axis=0))
            right = jnp.concatenate([parts[at, t] for t in range(p.u * p.hh)], axis=1)
            term = dot_t(jnp.concatenate(left, axis=1), right)
            value = term if value is None else value + term
        acc[...] += value
        return 0

    lax.fori_loop(0, p.NS // p.per, body, 0)
    full = acc[:, 0:LANES]
    for t in range(1, p.NR // LANES):
        full = full + acc[:, t * LANES : (t + 1) * LANES]
    full = fold(p, full)
    value = full[0 : p.HR, :]
    for b in range(1, p.hh):
        value = jnp.where(block_mask(p.RL, p.HR, b), full[b * p.HR : (b + 1) * p.HR, :], value)
    return value


def rest_kernel(p, parts, hot, mass_row, keep, acc):
    keep[0 : p.HR, :] = totals_of(p, parts, hot, acc, 0, lambda n: None)
    keep[p.HR :, :] = mass_row[...]


def step_scratch_of(p):
    return (
        pltpu.VMEM((p.F // LANES, 2 * p.RL, LANES), BF),
        pltpu.VMEM((p.J, p.RL, p.ML), F32),
        pltpu.VMEM((p.F // 2, p.NR), F32),
    )


def split_predicted(p, pred, pred_keep, pred_give):
    mine = (lax.axis_index("mkt") & 1) * p.PH
    pred_keep[...] = pred[pl.ds(pl.multiple_of(mine, 8), p.PH), :]
    pred_give[...] = pred[pl.ds(pl.multiple_of(p.PH - mine, 8), p.PH), :]


def first_kernel(
    p, table, mean_t, taste, hot, mass_t, mass_row, pred_keep, pred_give, parts, give, pred, *scratch
):
    step_body(p, table, mean_t, taste, hot, mass_t, mass_row, pred, parts, give, *scratch)
    split_predicted(p, pred, pred_keep, pred_give)


def update(p, recv, gap_mine, gap_other, table_in, mean_in, shift_t, table, mean_t):
    clip = clip_of(p, sum_chunks(p, recv, p.S2, p.PH, 1))
    mine = (lax.axis_index("grp") & 1) * p.HR
    for ref, start in ((gap_mine, mine), (gap_other, p.HR - mine)):
        at = pl.ds(pl.multiple_of(start, 8), p.HR)
        table[at, :] = table_in[at, :] + clip * ref[0 : p.HR, :]
    halves = []
    for side in range(2):
        total = recv[side * p.S2 : side * p.S2 + p.PH, :]
        for c in range(side + 2, p.C, 2):
            total = total + recv[c * p.S2 : c * p.S2 + p.PH, :]
        halves.append(total)
    total = jnp.log(jnp.concatenate(halves, axis=0))
    for b in range(p.hh):
        mean_t[b] = mean_in[b] + shift_t[b] - total[b * p.J : (b + 1) * p.J, :]


def next_kernel(
    p, recv, gap_mine, gap_other, table_in, mean_in, shift_t, taste, hot, mass_t, mass_row,
    table, mean_t, pred_keep, pred_give, parts, give, pred, *scratch
):
    update(p, recv, gap_mine, gap_other, table_in, mean_in, shift_t, table, mean_t)
    step_body(p, table, mean_t, taste, hot, mass_t, mass_row, pred, parts, give, *scratch)
    split_predicted(p, pred, pred_keep, pred_give)


def last_kernel(
    p, recv, gap_mine, gap_other, table_in, mean_in, shift_t, taste, hot, mass_t, mass_row,
    table, mean_t, pred, parts, give, *scratch
):
    update(p, recv, gap_mine, gap_other, table_in, mean_in, shift_t, table, mean_t)
    step_body(p, table, mean_t, taste, hot, mass_t, mass_row, pred, parts, give, *scratch)


def add_kernel(p, a, b, *refs):
    refs[len(refs) // 2][...] = a[...] + b[...]
    for n in range(len(refs) // 2):
        refs[len(refs) // 2 + 1 + n][...] = refs[n][...]


def gap_kernel(p, mine, other, share, *refs):
    gap = refs[-1] if len(refs) == 1 else refs[2]
    if len(refs) > 1:
        refs[3][...] = refs[0][...] + refs[1][...]
    total = mine[...] + other[...]
    at = pl.ds(pl.multiple_of((lax.axis_index("grp") & 1) * p.HR, 8), p.HR)
    value = jnp.log(share[at, :]) - jnp.log(total[0 : p.HR, :] / total[p.HR : p.HR + 1, :])
    gap[0 : p.HR, :] = value
    rows = jnp.sum(value * value, axis=0, keepdims=True)
    gap[p.HR :, :] = jnp.broadcast_to(jnp.sum(rows, axis=1, keepdims=True), (8, LANES))


def send_kernel(p, gap_mine, gap_other, pred, send):
    squares = gap_mine[p.HR :, :] + gap_other[p.HR :, :]
    value = pred[...]
    for c in range(p.C):
        send[c * p.S2 : c * p.S2 + p.PH, :] = value
        send[c * p.S2 + p.PH : (c + 1) * p.S2, :] = squares


def final_kernel(p, gap_mine, gap_other, table, columns, pred, mean_t, shift_t, send, own, gap, nat, means):
    mine = (lax.axis_index("grp") & 1) * p.HR
    for ref, start in ((gap_mine, mine), (gap_other, p.HR - mine)):
        gap[pl.ds(pl.multiple_of(start, 8), p.HR), :] = ref[0 : p.HR, :]
    squares = gap_mine[p.HR : p.HR + 1, :] + gap_other[p.HR : p.HR + 1, :]
    lane = lax.broadcasted_iota(jnp.int32, (LANES, LANES), 1).astype(F32)
    for n, ref in enumerate((table, gap)):
        pieces = jnp.concatenate(split3(ref[...]), axis=1)
        picked = None
        for o in range(p.hh):
            total = None
            for b in range(p.hh):
                wide = -(-p.FP // LANES)
                hot = [columns[o] == lane + float(b * p.FP + t * LANES) for t in range(wide)]
                hot = jnp.concatenate([x.astype(F32).astype(BF) for x in hot], axis=1)[:, 0 : p.FP]
                found = dot(hot, pieces)
                found = found[:, 0:LANES] + found[:, LANES : 2 * LANES] + found[:, 2 * LANES :]
                if p.hh > 1:
                    found = jnp.where(block_mask(p.RL, LANES, b), found, 0.0)
                total = found if total is None else total + found
            total = fold(p, total)
            picked = total if picked is None else jnp.where(block_mask(p.RL, LANES, o), total, picked)
        at = p.i8 + n * p.oi
        for c in range(p.C):
            send[c * p.S3 + at : c * p.S3 + at + p.oi, :] = picked[c * p.oi : (c + 1) * p.oi, :]
    tb = p.top // p.h

    def by_owner(block, store):
        if p.PR >= LANES:
            per = p.PR // LANES
            for gi in range(per):
                tall = [block(q * per + gi) for q in range(p.h)]
                nat[gi * LANES : (gi + 1) * LANES, :] = jnp.concatenate(tall, axis=0).T
        else:
            per = LANES // p.PR
            tall = [moved(block(q // per), -(q % per) * p.PR) for q in range(p.h)]
            nat[0:LANES, :] = jnp.concatenate(tall, axis=0).T
        for c in range(p.C):
            for a in range(tb):
                at = (a * p.C + c) * p.w
                store(c, slice(a * p.w, (a + 1) * p.w), nat[at : at + p.w, :])

    def put_mean(c, at, value):
        means[c, at, :] = value

    def put_pred(c, at, value):
        send[c * p.S3 + at.start : c * p.S3 + at.stop, :] = value

    by_owner(lambda b: mean_t[b] + shift_t[b], put_mean)
    by_owner(lambda b: pred[b * p.J : (b + 1) * p.J, :], put_pred)
    own[...] = means[lax.axis_index("mkt")]
    for c in range(p.C):
        send[(c + 1) * p.S3 - 1 : (c + 1) * p.S3, :] = squares


def out_kernel(p, recv, own, mean_out, loyalty_out):
    predicted = sum_chunks(p, recv, p.S3, 0, p.i8)
    value = own[...] - jnp.log(predicted)
    for q in range(p.h):
        mean_out[q * p.i8 : (q + 1) * p.i8, :] = moved(value, -q * p.J)[:, 0 : p.J]
    clip = clip_of(p, sum_chunks(p, recv, p.S3, p.S3 - 1, 1))
    for t in range(p.R // LANES):
        values = []
        for b in range(p.hh):
            at = (t * p.hh + b) * p.S3 + p.i8
            values.append(recv[at : at + p.oi, :] + clip * recv[at + p.oi : at + 2 * p.oi, :])
        for o in range(p.hh):
            row = moved(values[0], -o * p.RL)
            for b in range(1, p.hh):
                row = jnp.where(block_mask(p.RL, p.oi, b), moved(values[b], (b - o) * p.RL), row)
            loyalty_out[o * p.oi : (o + 1) * p.oi, t * LANES : (t + 1) * LANES] = row


def local(
    mean_utility,
    market_share,
    product_traits,
    taste_draws,
    taste_scale,
    type_weight,
    market_size,
    product_firm,
    firm_order,
    loyalty,
    firm_share,
):
    p = Plan(
        lax.axis_size("mkt"),
        lax.axis_size("grp"),
        mean_utility.shape[0],
        mean_utility.shape[1],
        taste_scale.shape[0],
        firm_share.shape[1],
        firm_share.shape[0],
        loyalty.shape[0],
    )

    def exchange(x):
        return lax.all_to_all(x, "mkt", split_axis=0, concat_axis=0, tiled=True)

    def swap(x, bit):
        return lax.ppermute(x, "grp", [(q, q ^ bit) for q in range(p.Q)])

    order = firm_order.reshape(p.C, p.Q, p.own)
    order = jnp.pad(order, ((0, 0), (0, 0), (0, p.ownp - p.own)), constant_values=-1)
    order = order.reshape(p.C, p.Q, p.hh, p.oi).transpose(1, 2, 0, 3).reshape(p.Q * p.hh, p.C * p.oi)
    order = jnp.pad(order, ((0, 0), (0, LANES - p.C * p.oi)), constant_values=-1)
    if p.ownp > p.own:
        loyalty = jnp.pad(loyalty, ((0, p.ownp - p.own), (0, 0)))

    send = call(
        p,
        pack_kernel,
        sds((p.C * p.S, LANES)),
        (
            taste_scale,
            market_size,
            taste_draws.transpose(1, 0, 2),
            type_weight,
            loyalty,
            product_traits.transpose(2, 0, 1),
            product_firm,
            mean_utility,
            market_share,
        ),
        vmem=60,
        specs=[HBM] * 9,
        out_specs=HBM,
        scratch=(
            pltpu.VMEM((p.K, p.M, p.R), F32),
            pltpu.VMEM((p.M, p.R), F32),
            pltpu.VMEM((p.ownp, p.R), F32),
            pltpu.VMEM((p.K, p.M, p.J), F32),
            pltpu.VMEM((p.M, p.J), jnp.int32),
            pltpu.VMEM((p.M, p.J), F32),
            pltpu.VMEM((p.M, p.J), F32),
            pltpu.VMEM((p.C * p.S, LANES), F32),
            pltpu.SMEM((p.K,), F32),
            pltpu.SMEM((p.M,), F32),
            pltpu.SemaphoreType.DMA((9,)),
            pltpu.SemaphoreType.DMA((p.C,)),
        ),
    )
    tiles = sds((p.hh, p.J, LANES))
    firms_t, mean_t, shift_t, mass_t, mass_row, loy, draws_t, traits_t = call(
        p,
        prep_kernel,
        (
            tiles,
            tiles,
            tiles,
            sds((p.RL, p.ML)),
            sds((8, LANES)),
            sds((LANES, LANES)),
            sds((p.K, p.RL, p.ML)),
            sds((p.K, p.hh, p.J, LANES)),
        ),
        (exchange(send),),
        scratch=(pltpu.VMEM((max(LANES, p.PR), LANES), F32),),
    )
    rows = [loy] + [swap(loy, bits) for bits in range(1, p.Q)]
    taste, hot = call(
        p,
        taste_kernel,
        (sds((p.J, p.RL, p.ML)), sds((p.J, p.hh, p.F, LANES), BF)),
        (draws_t, traits_t, firms_t),
    )
    table, share, columns = call(
        p,
        table_kernel,
        (sds((p.FP, LANES)), sds((p.FP, LANES)), sds((p.hh, LANES, LANES))),
        (order, firm_share, *rows),
        specs=[VM, HBM] + [VM] * len(rows),
        scratch=(pltpu.VMEM((p.F, LANES), F32), pltpu.SemaphoreType.DMA(())),
    )
    half = sds((p.HR + 8, LANES))
    tables = (sds((p.FP, LANES)), tiles)
    half_pred = sds((p.PH, LANES))
    all_parts = sds((p.NS, p.u * p.hh, p.NR, LANES), BF)
    step_scratch = step_scratch_of(p)
    whole_pred = (pltpu.VMEM((p.PB, LANES), F32),)
    fixed = (taste, hot, mass_t, mass_row)
    for step in range(ITERS):
        last = step == ITERS - 1
        if step == 0:
            pred, pred_give, parts, give = call(
                p,
                first_kernel,
                (half_pred, half_pred, all_parts, half),
                (table, mean_t, *fixed),
                scratch=whole_pred + step_scratch,
            )
        elif not last:
            table, mean_t, pred, pred_give, parts, give = call(
                p,
                next_kernel,
                tables + (half_pred, half_pred, all_parts, half),
                (recv, gap_mine, gap_other, table, mean_t, shift_t, *fixed),
                scratch=whole_pred + step_scratch,
            )
        else:
            table, mean_t, pred, parts, give = call(
                p,
                last_kernel,
                tables + (sds((p.PB, LANES)), all_parts, half),
                (recv, gap_mine, gap_other, table, mean_t, shift_t, *fixed),
                scratch=step_scratch,
            )
        given = swap(give, 1)
        keep = call(p, rest_kernel, half, (parts, hot, mass_row), scratch=step_scratch[-1:])
        if last:
            (mine,) = call(p, add_kernel, (half,), (keep, given))
        else:
            mine, pred_give = call(p, add_kernel, (half, half_pred), (keep, given, pred_give))
            pred_other = lax.ppermute(pred_give, "mkt", [(c, c ^ 1) for c in range(p.C)])
        bit = 2
        while 2 * bit < p.Q:
            (mine,) = call(p, add_kernel, (half,), (mine, swap(mine, bit)))
            bit *= 2
        sums = (mine, swap(mine, bit), share)
        if last:
            gap_mine = call(p, gap_kernel, half, sums)
        else:
            gap_mine, pred = call(p, gap_kernel, (half, half_pred), sums + (pred, pred_other))
        gap_other = swap(gap_mine, 1)
        if not last:
            recv = exchange(
                call(p, send_kernel, sds((p.C * p.S2, LANES)), (gap_mine, gap_other, pred))
            )
    send, own = call(
        p,
        final_kernel,
        (sds((p.C * p.S3, LANES)), sds((p.i8, LANES))),
        (gap_mine, gap_other, table, columns, pred, mean_t, shift_t),
        scratch=(
            pltpu.VMEM((p.FP, LANES), F32),
            pltpu.VMEM((max(LANES, p.PR), LANES), F32),
            pltpu.VMEM((p.C, p.i8, LANES), F32),
        ),
    )
    mean_out, loyalty_out = call(
        p, out_kernel, (sds((p.M, p.J)), sds((p.ownp, p.R))), (exchange(send), own)
    )
    return (mean_out, loyalty_out[0 : p.own] if p.ownp > p.own else loyalty_out)


def solution(mesh):
    both = ("mkt", "grp")
    placed = (
        P(both, None),
        P(both, None),
        P(both, None, None),
        P(both, None, None),
        P(),
        P(both, None),
        P(both),
        P(both, None),
        P(),
        P(both, None),
        P(),
    )
    return jax.shard_map(
        local,
        mesh=mesh,
        in_specs=placed,
        out_specs=(P(both, None), P(both, None)),
        check_vma=False,
    )
```

```python
import functools

import jax
import jax.numpy as jnp
from jax import lax
from jax.experimental import pallas as pl
from jax.experimental.pallas import tpu as pltpu
from jax.sharding import PartitionSpec as P

ITERS = 3
LANES = 128
clip_target = 0.5
norm_eps = 1e-06
BF = jnp.bfloat16
F32 = jnp.float32


class Plan:
    def __init__(self, mkt, grp, own_markets, products, traits, types, firms, own_firms):
        self.C, self.Q = mkt, grp
        self.M, self.J, self.K = own_markets, products, traits
        self.R, self.F, self.own = types, firms, own_firms
        self.RL = types // mkt
        self.hh = LANES // self.RL
        self.ii = own_markets // self.hh
        self.h = LANES // products
        self.i8 = own_markets // self.h
        self.top = max(self.hh, self.h)
        self.w = own_markets // self.top
        self.ML = own_markets * mkt
        self.PR = mkt * self.i8
        self.FP = firms // self.hh
        self.HR = self.FP // 2
        self.ownp = -(-own_firms // self.hh) * self.hh
        self.oi = self.ownp // self.hh
        self.u = max(1, 256 // self.ML)
        self.NS = products // self.u
        self.per = self.NS if self.NS <= 32 else 16
        self.plain = self.hh == 1 and mkt * own_firms == LANES and LANES % (grp * own_firms) == 0
        self.NR = max(LANES, 2 * self.RL)
        self.s_draws = 0
        self.s_mass = self.s_draws + traits * self.ii
        self.s_loy = self.s_mass + self.ii
        self.s_traits = self.s_loy + self.oi
        self.s_firms = self.s_traits + traits * self.i8
        self.s_mean = self.s_firms + self.i8
        self.s_shift = self.s_mean + self.i8
        self.S = -(-(self.s_shift + self.i8) // 8) * 8
        self.PB = self.hh * products
        self.PH = self.PB // 2
        self.S2 = self.PH + 8
        self.S3 = -(-(self.i8 + 2 * self.oi + 1) // 8) * 8
        self.vmem = 16 if firms * products * self.ML <= 2**22 else 58


VM = pl.BlockSpec(memory_space=pltpu.VMEM)
HBM = pl.BlockSpec(memory_space=pltpu.HBM)


def call(p, kernel, outs, args, scratch=(), specs=None, out_specs=None, vmem=None):
    return pl.pallas_call(
        functools.partial(kernel, p),
        out_shape=outs,
        in_specs=specs or [VM] * len(args),
        out_specs=out_specs or jax.tree.map(lambda _: VM, outs),
        scratch_shapes=list(scratch),
        compiler_params=pltpu.CompilerParams(vmem_limit_bytes=(vmem or p.vmem) * 2**20),
    )(*args)


def sds(shape, dtype=F32):
    return jax.ShapeDtypeStruct(shape, dtype)


def block_mask(width, rows, b):
    return lax.broadcasted_iota(jnp.int32, (rows, LANES), 1) // width == b


def fold(p, x):
    total = x
    for b in range(1, p.hh):
        total = total + pltpu.roll(x, b * p.RL, 1)
    return total


def split2(x):
    a = x.astype(BF)
    return a, (x - a.astype(F32)).astype(BF)


def split3(x):
    a = x.astype(BF)
    b, c = split2(x - a.astype(F32))
    return a, b, c


def dot(a, b):
    return jnp.dot(a, b, preferred_element_type=F32)


def dot_t(a, b):
    return lax.dot_general(a, b, (((1,), (1,)), ((), ())), preferred_element_type=F32)


def moved(x, shift):
    return pltpu.roll(x, shift % LANES, 1) if shift % LANES else x


def pack_kernel(
    p, scale_h, size_h, draws_h, weight_h, loyalty_h, traits_h, firms_h, mean_h, share_h, out_h,
    draws, weight, loyalty, traits, firms, mean, share, out, scale, size, sems, out_sems,
):
    pairs = (
        (draws_h, draws), (weight_h, weight), (traits_h, traits), (firms_h, firms),
        (mean_h, mean), (share_h, share), (loyalty_h, loyalty), (scale_h, scale), (size_h, size),
    )
    copies = [pltpu.make_async_copy(a, b, sems.at[n]) for n, (a, b) in enumerate(pairs)]
    for copy in copies:
        copy.start()
    for copy in copies:
        copy.wait()
    row = lax.broadcasted_iota(jnp.int32, (p.M, LANES), 0)
    column = jnp.zeros((p.M, LANES), F32)
    for m in range(p.M):
        column = jnp.where(row == m, size[m], column)
    mass_total = None
    tiles = []
    for t in range(p.R // LANES):
        tile = weight[:, t * LANES : (t + 1) * LANES] * column
        tiles.append(tile)
        mass_total = tile if mass_total is None else mass_total + tile
    mass_total = jnp.sum(mass_total, axis=1, keepdims=True)

    def by_type(tile_of, c, section, rows):
        tile, b = tile_of(c // p.hh), c % p.hh
        value = tile[0:rows, :] if not b else moved(tile, -b * p.RL)[0:rows, :]
        for q in range(1, p.hh):
            piece = moved(tile, (q - b) * p.RL)[q * rows : (q + 1) * rows, :]
            value = jnp.where(block_mask(p.RL, rows, q), piece, value)
        out[c * p.S + section : c * p.S + section + rows, :] = value

    def packed(x):
        return jnp.concatenate([x[q * p.i8 : (q + 1) * p.i8, :] for q in range(p.h)], axis=1)

    products = [packed(traits[k] * scale[k]) for k in range(p.K)]
    products += [packed(firms[...].astype(F32)), packed(mean[...])]
    products += [packed(jnp.log(share[...]) + jnp.log(mass_total))]
    sends = []
    for c in range(p.C):
        for k in range(p.K):
            by_type(lambda t: draws[k, :, t * LANES : (t + 1) * LANES], c, p.s_draws + k * p.ii, p.ii)
        by_type(lambda t: tiles[t], c, p.s_mass, p.ii)
        by_type(lambda t: loyalty[:, t * LANES : (t + 1) * LANES], c, p.s_loy, p.oi)
        for n, value in enumerate(products):
            at = c * p.S + p.s_traits + n * p.i8
            out[at : at + p.i8, :] = value
        part = pl.ds(c * p.S, p.S)
        copy = pltpu.make_async_copy(out.at[part], out_h.at[part], out_sems.at[c])
        copy.start()
        sends.append(copy)
    for copy in sends:
        copy.wait()


def prep_kernel(p, recv, firms_t, mean_t, shift_t, mass_t, mass_row, loy, draws_t, traits_t, nat):
    ta = p.top // p.hh

    def typed(section, store):
        for a in range(ta):
            for c in range(p.C):
                at = c * p.S + section + a * p.w
                nat[(a * p.C + c) * p.w : (a * p.C + c + 1) * p.w, :] = recv[at : at + p.w, :]
        flat = nat[0:LANES, :]
        turned = flat.T
        for b in range(p.hh):
            store(b, turned[b * p.RL : (b + 1) * p.RL, :])
        return flat

    def put_mass(b, value):
        mass_t[:, b * LANES : (b + 1) * LANES] = value

    flat = typed(p.s_mass, put_mass)
    row = jnp.sum(flat, axis=0, keepdims=True)
    mass_row[...] = fold(p, jnp.broadcast_to(row, (8, LANES)))
    for k in range(p.K):

        def put_draws(b, value):
            draws_t[k, :, b * LANES : (b + 1) * LANES] = value

        typed(p.s_draws + k * p.ii, put_draws)

    tb = p.top // p.h

    def product(section, store):
        for copy in range(max(1, LANES // p.PR)):
            for a in range(tb):
                for c in range(p.C):
                    at = c * p.S + section + a * p.w
                    to = copy * p.PR + (a * p.C + c) * p.w
                    nat[to : to + p.w, :] = recv[at : at + p.w, :]
        if p.PR >= LANES:
            per = p.PR // LANES
            for gi in range(per):
                turned = nat[gi * LANES : (gi + 1) * LANES, :].T
                for q in range(p.h):
                    store(q * per + gi, turned[q * p.J : (q + 1) * p.J, :])
        else:
            per = LANES // p.PR
            turned = nat[0:LANES, :].T
            for b in range(p.hh):
                value = turned[b * per * p.J : (b * per + 1) * p.J, :]
                for s in range(1, per):
                    at = (b * per + s) * p.J
                    value = jnp.where(block_mask(p.PR, p.J, s), turned[at : at + p.J, :], value)
                store(b, value)

    def into(ref):
        def store(b, value):
            ref[b] = value

        return store

    product(p.s_firms, into(firms_t))
    product(p.s_mean, into(mean_t))
    product(p.s_shift, into(shift_t))
    for k in range(p.K):
        product(p.s_traits + k * p.i8, into(traits_t.at[k]))
    loy[...] = jnp.zeros_like(loy)
    for c in range(p.C):
        loy[c * p.oi : (c + 1) * p.oi, :] = recv[c * p.S + p.s_loy : c * p.S + p.s_loy + p.oi, :]


def taste_kernel(p, draws_t, traits_t, firms_t, order_in, taste, hot, order):
    if p.plain:
        spread = [jnp.broadcast_to(order_in[n : n + 1, :], (8, LANES)) for n in range(p.F // LANES)]
        for q in range(p.Q):
            row = None
            for c in range(p.C):
                n, at = divmod((c * p.Q + q) * p.own, LANES)
                piece = moved(spread[n], c * p.own - at)
                row = piece if row is None else jnp.where(block_mask(p.own, 8, c), piece, row)
            order[q : q + 1, :] = row[0:1, :]
    else:
        order[...] = order_in[...]
    rows = min(p.F, 256)
    firm = lax.broadcasted_iota(jnp.int32, (rows, LANES), 0).astype(F32).astype(BF)

    def body(n, _):
        for v in range(p.u):
            j = n * p.u + v
            for b in range(p.hh):
                at = slice(b * LANES, (b + 1) * LANES)
                value = None
                for k in range(p.K):
                    term = traits_t[k, b, pl.ds(j, 1), :] * draws_t[k, :, at]
                    value = term if value is None else value + term
                taste[j, :, at] = value
                row = firms_t[b, pl.ds(j, 1), :]
                for base in range(0, p.F, rows):
                    want = jnp.broadcast_to(row - float(base), (rows, LANES)).astype(BF)
                    hot[j, b, base : base + rows, :] = jnp.where(firm == want, jnp.ones((), BF), jnp.zeros((), BF))
        return 0

    lax.fori_loop(0, p.NS, body, 0)


def table_kernel(p, order, share_h, *refs):
    blocks, (table, share, columns, tile, sem) = refs[:-5], refs[-5:]
    lane = lax.axis_index("mkt") * p.RL
    start = pl.multiple_of(lane // LANES * LANES, LANES)
    copy = pltpu.make_async_copy(share_h.at[:, pl.ds(start, LANES)], tile, sem)
    copy.start()
    firm = lax.broadcasted_iota(jnp.int32, (p.F, LANES), 0)
    total = jnp.zeros((p.F, LANES), F32)
    blocks = [ref[at : at + LANES, :] for ref in blocks for at in range(0, ref.shape[0], LANES)]
    for s, block in enumerate(blocks):
        pieces = jnp.concatenate(split3(block), axis=1)
        member = lax.axis_index("grp") ^ s
        for b in range(p.hh):
            hot = (firm == order[pl.ds(member * p.hh + b, 1), :]).astype(F32).astype(BF)
            found = dot(hot, pieces)
            found = found[:, 0:LANES] + found[:, LANES : 2 * LANES] + found[:, 2 * LANES :]
            if p.hh > 1:
                found = jnp.where(block_mask(p.RL, p.F, b), found, 0.0)
            total = total + found
    pack_table(p, fold(p, total), table)
    for b in range(p.hh):
        row = order[pl.ds(lax.axis_index("grp") * p.hh + b, 1), :].astype(F32)
        columns[b] = jnp.broadcast_to(row, (LANES, LANES)).T
    copy.wait()
    if p.hh == 1:
        share[...] = tile[...]
    else:
        for b in range(p.hh):
            part = pltpu.roll(tile[b * p.FP : (b + 1) * p.FP, :], (b * p.RL + LANES - (lane - start)) % LANES, 1)
            mask = block_mask(p.RL, p.FP, b)
            share[...] = part if not b else jnp.where(mask, part, share[...])


def pack_table(p, full, out):
    value = full[0 : p.FP, :]
    for b in range(1, p.hh):
        value = jnp.where(block_mask(p.RL, p.FP, b), full[b * p.FP : (b + 1) * p.FP, :], value)
    out[...] = value


def clip_of(p, squares):
    return jnp.minimum(1.0, clip_target / jnp.sqrt(squares / (p.F * p.R) + norm_eps))


def sum_chunks(p, recv, step, start, rows):
    total = recv[start : start + rows, :]
    for c in range(1, p.C):
        total = total + recv[c * step + start : c * step + start + rows, :]
    return total


def step_body(p, table, mean_of, taste, hot, mass_t, mass_row, pred, parts, give, tab, expu, acc):
    turned = table[...].T
    for q, piece in enumerate(split2(turned)):
        for t in range(p.F // LANES):
            b, at = divmod(t * LANES, p.FP)
            tab[t, q * p.RL : (q + 1) * p.RL, :] = piece[b * p.RL : (b + 1) * p.RL, at : at + LANES]

    def hot_of(n):
        return jnp.concatenate([hot[n * p.u + v, b] for v in range(p.u) for b in range(p.hh)], axis=1)

    def gather(n, total):
        found = dot(jnp.concatenate([tab[t] for t in range(p.F // LANES)], axis=1), hot_of(n))
        found = found[0 : p.RL] + found[p.RL : 2 * p.RL]
        for v in range(p.u):
            j = n * p.u + v
            means = [jnp.broadcast_to(mean_of[b, pl.ds(j, 1), :], (p.RL, LANES)) for b in range(p.hh)]
            means = means[0] if p.hh == 1 else jnp.concatenate(means, axis=1)
            e = jnp.exp(taste[j] + found[:, v * p.ML : (v + 1) * p.ML] + means)
            expu[j] = e
            total = total + e
        return total

    total = lax.fori_loop(0, p.NS, gather, jnp.zeros((p.RL, p.ML), F32), unroll=min(16, p.NS))
    scale = mass_t[...] / (1.0 + total)
    if p.NR > 2 * p.RL:
        parts[...] = jnp.zeros_like(parts)

    def fill(n):
        for v in range(p.u):
            j = n * p.u + v
            x = expu[j] * scale
            hi, lo = split2(x)
            for b in range(p.hh):
                at = slice(b * LANES, (b + 1) * LANES)
                parts[n, v * p.hh + b, 0 : p.RL, :] = hi[:, at]
                parts[n, v * p.hh + b, p.RL : 2 * p.RL, :] = lo[:, at]
            row = jnp.sum(x, axis=0, keepdims=True)
            for b in range(p.hh):
                pred[pl.ds(b * p.J + j, 1), :] = row[:, b * LANES : (b + 1) * LANES]

    give[0 : p.HR, :] = totals_of(p, parts, hot, acc, 1, fill)
    give[p.HR :, :] = mass_row[...]


def totals_of(p, parts, hot, acc, other, fill):
    start = ((lax.axis_index("grp") & 1) ^ other) * p.HR
    acc[...] = jnp.zeros_like(acc)

    def body(n, _):
        value = None
        for s in range(p.per):
            at = n * p.per + s
            fill(at)
            left = []
            for v in range(p.u):
                for b in range(p.hh):
                    rows = [pl.ds(pl.multiple_of(start + fh * p.FP, 8), p.HR) for fh in range(p.hh)]
                    tall = [hot[at * p.u + v, b, r, :] for r in rows]
                    left.append(tall[0] if p.hh == 1 else jnp.concatenate(tall, axis=0))
            right = jnp.concatenate([parts[at, t] for t in range(p.u * p.hh)], axis=1)
            term = dot_t(jnp.concatenate(left, axis=1), right)
            value = term if value is None else value + term
        acc[...] += value
        return 0

    lax.fori_loop(0, p.NS // p.per, body, 0)
    full = acc[:, 0:LANES]
    for t in range(1, p.NR // LANES):
        full = full + acc[:, t * LANES : (t + 1) * LANES]
    full = fold(p, full)
    value = full[0 : p.HR, :]
    for b in range(1, p.hh):
        value = jnp.where(block_mask(p.RL, p.HR, b), full[b * p.HR : (b + 1) * p.HR, :], value)
    return value


def rest_kernel(p, parts, hot, mass_row, keep, acc):
    keep[0 : p.HR, :] = totals_of(p, parts, hot, acc, 0, lambda n: None)
    keep[p.HR :, :] = mass_row[...]


def step_scratch_of(p):
    return (
        pltpu.VMEM((p.F // LANES, 2 * p.RL, LANES), BF),
        pltpu.VMEM((p.J, p.RL, p.ML), F32),
        pltpu.VMEM((p.F // 2, p.NR), F32),
    )


def split_predicted(p, pred, pred_keep, pred_give):
    mine = (lax.axis_index("mkt") & 1) * p.PH
    pred_keep[...] = pred[pl.ds(pl.multiple_of(mine, 8), p.PH), :]
    pred_give[...] = pred[pl.ds(pl.multiple_of(p.PH - mine, 8), p.PH), :]


def first_kernel(
    p, table, mean_t, taste, hot, mass_t, mass_row, pred_keep, pred_give, parts, give, pred, *scratch
):
    step_body(p, table, mean_t, taste, hot, mass_t, mass_row, pred, parts, give, *scratch)
    split_predicted(p, pred, pred_keep, pred_give)


def update(p, recv, gap_mine, gap_other, table_in, mean_in, shift_t, table, mean_t):
    clip = clip_of(p, sum_chunks(p, recv, p.S2, p.PH, 1))
    mine = (lax.axis_index("grp") & 1) * p.HR
    for ref, start in ((gap_mine, mine), (gap_other, p.HR - mine)):
        at = pl.ds(pl.multiple_of(start, 8), p.HR)
        table[at, :] = table_in[at, :] + clip * ref[0 : p.HR, :]
    halves = []
    for side in range(2):
        total = recv[side * p.S2 : side * p.S2 + p.PH, :]
        for c in range(side + 2, p.C, 2):
            total = total + recv[c * p.S2 : c * p.S2 + p.PH, :]
        halves.append(total)
    total = jnp.log(jnp.concatenate(halves, axis=0))
    for b in range(p.hh):
        mean_t[b] = mean_in[b] + shift_t[b] - total[b * p.J : (b + 1) * p.J, :]


def next_kernel(
    p, recv, gap_mine, gap_other, table_in, mean_in, shift_t, taste, hot, mass_t, mass_row,
    table, mean_t, pred_keep, pred_give, parts, give, pred, *scratch
):
    update(p, recv, gap_mine, gap_other, table_in, mean_in, shift_t, table, mean_t)
    step_body(p, table, mean_t, taste, hot, mass_t, mass_row, pred, parts, give, *scratch)
    split_predicted(p, pred, pred_keep, pred_give)


def last_kernel(
    p, recv, gap_mine, gap_other, table_in, mean_in, shift_t, taste, hot, mass_t, mass_row,
    table, mean_t, pred, parts, give, *scratch
):
    update(p, recv, gap_mine, gap_other, table_in, mean_in, shift_t, table, mean_t)
    step_body(p, table, mean_t, taste, hot, mass_t, mass_row, pred, parts, give, *scratch)


def add_kernel(p, a, b, *refs):
    refs[len(refs) // 2][...] = a[...] + b[...]
    for n in range(len(refs) // 2):
        refs[len(refs) // 2 + 1 + n][...] = refs[n][...]


def gap_kernel(p, mine, other, share, *refs):
    gap = refs[-1] if len(refs) == 1 else refs[2]
    if len(refs) > 1:
        refs[3][...] = refs[0][...] + refs[1][...]
    total = mine[...] + other[...]
    at = pl.ds(pl.multiple_of((lax.axis_index("grp") & 1) * p.HR, 8), p.HR)
    value = jnp.log(share[at, :]) - jnp.log(total[0 : p.HR, :] / total[p.HR : p.HR + 1, :])
    gap[0 : p.HR, :] = value
    rows = jnp.sum(value * value, axis=0, keepdims=True)
    gap[p.HR :, :] = jnp.broadcast_to(jnp.sum(rows, axis=1, keepdims=True), (8, LANES))


def send_kernel(p, gap_mine, gap_other, pred, send):
    squares = gap_mine[p.HR :, :] + gap_other[p.HR :, :]
    value = pred[...]
    for c in range(p.C):
        send[c * p.S2 : c * p.S2 + p.PH, :] = value
        send[c * p.S2 + p.PH : (c + 1) * p.S2, :] = squares


def final_kernel(p, gap_mine, gap_other, table, columns, pred, mean_t, shift_t, send, own, gap, nat, means):
    mine = (lax.axis_index("grp") & 1) * p.HR
    for ref, start in ((gap_mine, mine), (gap_other, p.HR - mine)):
        gap[pl.ds(pl.multiple_of(start, 8), p.HR), :] = ref[0 : p.HR, :]
    squares = gap_mine[p.HR : p.HR + 1, :] + gap_other[p.HR : p.HR + 1, :]
    lane = lax.broadcasted_iota(jnp.int32, (LANES, LANES), 1).astype(F32)
    for n, ref in enumerate((table, gap)):
        pieces = jnp.concatenate(split3(ref[...]), axis=1)
        picked = None
        for o in range(p.hh):
            total = None
            for b in range(p.hh):
                wide = -(-p.FP // LANES)
                hot = [columns[o] == lane + float(b * p.FP + t * LANES) for t in range(wide)]
                hot = jnp.concatenate([x.astype(F32).astype(BF) for x in hot], axis=1)[:, 0 : p.FP]
                found = dot(hot, pieces)
                found = found[:, 0:LANES] + found[:, LANES : 2 * LANES] + found[:, 2 * LANES :]
                if p.hh > 1:
                    found = jnp.where(block_mask(p.RL, LANES, b), found, 0.0)
                total = found if total is None else total + found
            total = fold(p, total)
            picked = total if picked is None else jnp.where(block_mask(p.RL, LANES, o), total, picked)
        at = p.i8 + n * p.oi
        for c in range(p.C):
            send[c * p.S3 + at : c * p.S3 + at + p.oi, :] = picked[c * p.oi : (c + 1) * p.oi, :]
    tb = p.top // p.h

    def by_owner(block, store):
        if p.PR >= LANES:
            per = p.PR // LANES
            for gi in range(per):
                tall = [block(q * per + gi) for q in range(p.h)]
                nat[gi * LANES : (gi + 1) * LANES, :] = jnp.concatenate(tall, axis=0).T
        else:
            per = LANES // p.PR
            tall = [moved(block(q // per), -(q % per) * p.PR) for q in range(p.h)]
            nat[0:LANES, :] = jnp.concatenate(tall, axis=0).T
        for c in range(p.C):
            for a in range(tb):
                at = (a * p.C + c) * p.w
                store(c, slice(a * p.w, (a + 1) * p.w), nat[at : at + p.w, :])

    def put_mean(c, at, value):
        means[c, at, :] = value

    def put_pred(c, at, value):
        send[c * p.S3 + at.start : c * p.S3 + at.stop, :] = value

    by_owner(lambda b: mean_t[b] + shift_t[b], put_mean)
    by_owner(lambda b: pred[b * p.J : (b + 1) * p.J, :], put_pred)
    own[...] = means[lax.axis_index("mkt")]
    for c in range(p.C):
        send[(c + 1) * p.S3 - 1 : (c + 1) * p.S3, :] = squares


def out_kernel(p, recv, own, mean_out, loyalty_out):
    predicted = sum_chunks(p, recv, p.S3, 0, p.i8)
    value = own[...] - jnp.log(predicted)
    for q in range(p.h):
        mean_out[q * p.i8 : (q + 1) * p.i8, :] = moved(value, -q * p.J)[:, 0 : p.J]
    clip = clip_of(p, sum_chunks(p, recv, p.S3, p.S3 - 1, 1))
    for t in range(p.R // LANES):
        values = []
        for b in range(p.hh):
            at = (t * p.hh + b) * p.S3 + p.i8
            values.append(recv[at : at + p.oi, :] + clip * recv[at + p.oi : at + 2 * p.oi, :])
        for o in range(p.hh):
            row = moved(values[0], -o * p.RL)
            for b in range(1, p.hh):
                row = jnp.where(block_mask(p.RL, p.oi, b), moved(values[b], (b - o) * p.RL), row)
            loyalty_out[o * p.oi : (o + 1) * p.oi, t * LANES : (t + 1) * LANES] = row


def local(
    mean_utility,
    market_share,
    product_traits,
    taste_draws,
    taste_scale,
    type_weight,
    market_size,
    product_firm,
    firm_order,
    loyalty,
    firm_share,
):
    p = Plan(
        lax.axis_size("mkt"),
        lax.axis_size("grp"),
        mean_utility.shape[0],
        mean_utility.shape[1],
        taste_scale.shape[0],
        firm_share.shape[1],
        firm_share.shape[0],
        loyalty.shape[0],
    )

    def exchange(x):
        return lax.all_to_all(x, "mkt", split_axis=0, concat_axis=0, tiled=True)

    def swap(x, bit):
        return lax.ppermute(x, "grp", [(q, q ^ bit) for q in range(p.Q)])

    if p.plain:
        order = firm_order.reshape(p.F // LANES, LANES)
    else:
        order = firm_order.reshape(p.C, p.Q, p.own)
        order = jnp.pad(order, ((0, 0), (0, 0), (0, p.ownp - p.own)), constant_values=-1)
        order = order.reshape(p.C, p.Q, p.hh, p.oi).transpose(1, 2, 0, 3).reshape(p.Q * p.hh, p.C * p.oi)
        order = jnp.pad(order, ((0, 0), (0, LANES - p.C * p.oi)), constant_values=-1)
    if p.ownp > p.own:
        loyalty = jnp.pad(loyalty, ((0, p.ownp - p.own), (0, 0)))

    send = call(
        p,
        pack_kernel,
        sds((p.C * p.S, LANES)),
        (
            taste_scale,
            market_size,
            taste_draws.transpose(1, 0, 2),
            type_weight,
            loyalty,
            product_traits.transpose(2, 0, 1),
            product_firm,
            mean_utility,
            market_share,
        ),
        vmem=60,
        specs=[HBM] * 9,
        out_specs=HBM,
        scratch=(
            pltpu.VMEM((p.K, p.M, p.R), F32),
            pltpu.VMEM((p.M, p.R), F32),
            pltpu.VMEM((p.ownp, p.R), F32),
            pltpu.VMEM((p.K, p.M, p.J), F32),
            pltpu.VMEM((p.M, p.J), jnp.int32),
            pltpu.VMEM((p.M, p.J), F32),
            pltpu.VMEM((p.M, p.J), F32),
            pltpu.VMEM((p.C * p.S, LANES), F32),
            pltpu.SMEM((p.K,), F32),
            pltpu.SMEM((p.M,), F32),
            pltpu.SemaphoreType.DMA((9,)),
            pltpu.SemaphoreType.DMA((p.C,)),
        ),
    )
    tiles = sds((p.hh, p.J, LANES))
    firms_t, mean_t, shift_t, mass_t, mass_row, loy, draws_t, traits_t = call(
        p,
        prep_kernel,
        (
            tiles,
            tiles,
            tiles,
            sds((p.RL, p.ML)),
            sds((8, LANES)),
            sds((LANES, LANES)),
            sds((p.K, p.RL, p.ML)),
            sds((p.K, p.hh, p.J, LANES)),
        ),
        (exchange(send),),
        scratch=(pltpu.VMEM((max(LANES, p.PR), LANES), F32),),
    )
    rows = [loy] + [swap(loy, bits) for bits in range(1, p.Q)]
    taste, hot, order = call(
        p,
        taste_kernel,
        (sds((p.J, p.RL, p.ML)), sds((p.J, p.hh, p.F, LANES), BF), sds((p.Q * p.hh, LANES), jnp.int32)),
        (draws_t, traits_t, firms_t, order),
    )
    table, share, columns = call(
        p,
        table_kernel,
        (sds((p.FP, LANES)), sds((p.FP, LANES)), sds((p.hh, LANES, LANES))),
        (order, firm_share, *rows),
        specs=[VM, HBM] + [VM] * len(rows),
        scratch=(pltpu.VMEM((p.F, LANES), F32), pltpu.SemaphoreType.DMA(())),
    )
    half = sds((p.HR + 8, LANES))
    tables = (sds((p.FP, LANES)), tiles)
    half_pred = sds((p.PH, LANES))
    all_parts = sds((p.NS, p.u * p.hh, p.NR, LANES), BF)
    step_scratch = step_scratch_of(p)
    whole_pred = (pltpu.VMEM((p.PB, LANES), F32),)
    fixed = (taste, hot, mass_t, mass_row)
    for step in range(ITERS):
        last = step == ITERS - 1
        if step == 0:
            pred, pred_give, parts, give = call(
                p,
                first_kernel,
                (half_pred, half_pred, all_parts, half),
                (table, mean_t, *fixed),
                scratch=whole_pred + step_scratch,
            )
        elif not last:
            table, mean_t, pred, pred_give, parts, give = call(
                p,
                next_kernel,
                tables + (half_pred, half_pred, all_parts, half),
                (recv, gap_mine, gap_other, table, mean_t, shift_t, *fixed),
                scratch=whole_pred + step_scratch,
            )
        else:
            table, mean_t, pred, parts, give = call(
                p,
                last_kernel,
                tables + (sds((p.PB, LANES)), all_parts, half),
                (recv, gap_mine, gap_other, table, mean_t, shift_t, *fixed),
                scratch=step_scratch,
            )
        given = swap(give, 1)
        keep = call(p, rest_kernel, half, (parts, hot, mass_row), scratch=step_scratch[-1:])
        if last:
            (mine,) = call(p, add_kernel, (half,), (keep, given))
        else:
            mine, pred_give = call(p, add_kernel, (half, half_pred), (keep, given, pred_give))
            pred_other = lax.ppermute(pred_give, "mkt", [(c, c ^ 1) for c in range(p.C)])
        bit = 2
        while 2 * bit < p.Q:
            (mine,) = call(p, add_kernel, (half,), (mine, swap(mine, bit)))
            bit *= 2
        sums = (mine, swap(mine, bit), share)
        if last:
            gap_mine = call(p, gap_kernel, half, sums)
        else:
            gap_mine, pred = call(p, gap_kernel, (half, half_pred), sums + (pred, pred_other))
        gap_other = swap(gap_mine, 1)
        if not last:
            recv = exchange(
                call(p, send_kernel, sds((p.C * p.S2, LANES)), (gap_mine, gap_other, pred))
            )
    send, own = call(
        p,
        final_kernel,
        (sds((p.C * p.S3, LANES)), sds((p.i8, LANES))),
        (gap_mine, gap_other, table, columns, pred, mean_t, shift_t),
        scratch=(
            pltpu.VMEM((p.FP, LANES), F32),
            pltpu.VMEM((max(LANES, p.PR), LANES), F32),
            pltpu.VMEM((p.C, p.i8, LANES), F32),
        ),
    )
    mean_out, loyalty_out = call(
        p, out_kernel, (sds((p.M, p.J)), sds((p.ownp, p.R))), (exchange(send), own)
    )
    return (mean_out, loyalty_out[0 : p.own] if p.ownp > p.own else loyalty_out)


def solution(mesh):
    both = ("mkt", "grp")
    placed = (
        P(both, None),
        P(both, None),
        P(both, None, None),
        P(both, None, None),
        P(),
        P(both, None),
        P(both),
        P(both, None),
        P(),
        P(both, None),
        P(),
    )
    return jax.shard_map(
        local,
        mesh=mesh,
        in_specs=placed,
        out_specs=(P(both, None), P(both, None)),
        check_vma=False,
    )
```
